256 devices in a mesh: ka: 64 (over z, x, y_lo), orb: 4 (over y_hi, core).
Axes of the slice: x: 4, y: 4 (y_hi: 2, y_lo: 2; y = y_hi * 2 + y_lo), z: 8, core: 2. Of those that a mesh axis runs over, the one named last changes fastest.
Arguments:
- fock: float32 [2, 256, 384, 384], P(None, 'ka', 'orb'), may hold values from -3 to 3, as said below
- potential: float32 [4, 48, 48], P(None, 'orb'), may hold values from -0.9 to 0.9
- chem_potential: float32 [1], replicated, may hold values from -1 to 1
- spectral_bound: float32 [1], replicated, may hold values from 5.5 to 8
- impurity_orbitals: int32 [384], replicated, may hold values from 0 to 383, each once
- potential_of: int32 [8], replicated, may hold values from 0 to 3
Outputs:
- density_cells: float32 [2, 256, 384, 384], P(None, 'ka', 'orb')
- fragment_density: float32 [2, 8, 48, 48], P(None, 'orb')
The draws below stay inside these ranges and needn't reach their ends.
Inputs may be any that keep to these rules, and one draw needn't show every extreme that they name: `impurity_orbitals`: every orbital appears once; entries f * 48 to (f + 1) * 48 - 1 are fragment f's orbitals. `fock`: for each k-point the real part is symmetric and the imaginary part antisymmetric.
All inputs are finite; a program needn't handle non-finite values.
Results may differ from the reference program's by a relative error of at most 0.0001.
Values sent between devices are 32-bit elements; how exact they have to be, the bound alone decides.
A program may use at most 64 MiB of HBM per device.

```python
import math
import jax
import jax.numpy as jnp
from jax import lax

NORB = 384
NIMP = 48
NPOT = 4
ITERS = 2
NFRAG = 8
K = 256


def draw_fock(key, part):
    keys = jax.random.split(key, 4)
    shape = (K, NORB, NORB)
    spread = 0.7 / math.sqrt(NORB)
    raw_real = jnp.clip(jax.random.normal(keys[0], shape, jnp.float32), -5.0, 5.0)
    raw_imag = jnp.clip(jax.random.normal(keys[1], shape, jnp.float32), -5.0, 5.0)
    onsite = jax.random.uniform(keys[3], (K, NORB), jnp.float32, -2.0, 2.0)
    sym_real = 0.5 * spread * (raw_real + jnp.swapaxes(raw_real, 1, 2))
    anti_imag = 0.5 * spread * (raw_imag - jnp.swapaxes(raw_imag, 1, 2))
    diag_eye = jnp.eye(NORB, dtype=jnp.float32)
    real_part = sym_real + onsite[:, :, None] * diag_eye[None]
    return jnp.stack([real_part, anti_imag])


def plant(result, stream_key, smallest, top_value):
    dims = result.shape
    spot = [jax.random.randint(jax.random.fold_in(stream_key, axis), (), 0, dims[axis]) for axis in range(len(dims))]
    result = result.at[tuple(spot)].set(smallest)
    longest = dims.index(max(dims))
    spot[longest] = (spot[longest] + 1) % dims[longest]
    return result.at[tuple(spot)].set(top_value)


def levels(own_key, dims, cuts, least, high):
    def one(position, parts):
        draws = jax.random.uniform(jax.random.fold_in(jax.random.fold_in(own_key, 6), position), (parts,), jnp.float32, least / len(cuts), high / len(cuts))
        return jnp.repeat(jnp.exp(draws), dims[position] // parts).reshape((-1,) + (1,) * (len(dims) - position - 1))

    factor_of = one(*cuts[0])
    for cut in cuts[1:]:
        factor_of = factor_of * one(*cut)
    return factor_of


def noise(stream_key, extent, scale, most, cuts=(), held_as=jnp.bfloat16):
    result = scale * jax.random.normal(stream_key, extent, jnp.float32)
    if cuts:
        result = result * levels(stream_key, extent, cuts, -0.22, 0.18)
    return jnp.clip(result, -most, most).astype(held_as)


def setup_inputs(seed: int = 0) -> dict:
    splits = jax.random.split(jax.random.key(seed), 7)
    return {
        "fock": draw_fock(jax.random.fold_in(splits[6], 71), 0),
        "potential": noise(splits[1], (NPOT, NIMP, NIMP), 0.15, 0.9, ((1, 4),), jnp.float32),
        "chem_potential": jnp.clip(jax.random.uniform(splits[2], (1,), jnp.float32, -1.0, 1.0), -1.0, 1.0),
        "spectral_bound": jnp.clip(jax.random.uniform(splits[3], (1,), jnp.float32, 5.5, 8.0), 5.5, 8.0),
        "impurity_orbitals": jax.random.permutation(splits[4], NORB).astype(jnp.int32),
        "potential_of": plant(jax.random.randint(splits[5], (NFRAG,), 0, NPOT), jax.random.fold_in(splits[5], 1), 0, NPOT - 1).astype(jnp.int32),
    }


def complex_product(left_real, left_imag, right_real, right_imag):
    def product(first, second):
        return jnp.dot(first, second, precision=lax.Precision.HIGHEST, preferred_element_type=jnp.float32)
    return (product(left_real, right_real) - product(left_imag, right_imag),
            product(left_real, right_imag) + product(left_imag, right_real))


def reference(fock, potential, chem_potential, spectral_bound, impurity_orbitals, potential_of):
    symmetric = 0.5 * (potential + jnp.swapaxes(potential, 1, 2))
    blocks = symmetric[potential_of]
    slots = impurity_orbitals.reshape(NFRAG, NIMP)
    shift = jnp.zeros((NORB, NORB), jnp.float32).at[slots[:, :, None], slots[:, None, :]].set(blocks)
    identity = jnp.eye(NORB, dtype=jnp.float32)
    level = chem_potential[0]
    scale = spectral_bound[0]

    def purify(matrix):
        sign_real = (matrix[0] + shift - level * identity) / scale
        sign_imag = matrix[1] / scale
        for step in range(ITERS):
            square_real, square_imag = complex_product(sign_real, sign_imag, sign_real, sign_imag)
            cube_real, cube_imag = complex_product(square_real, square_imag, sign_real, sign_imag)
            sign_real = 1.5 * sign_real - 0.5 * cube_real
            sign_imag = 1.5 * sign_imag - 0.5 * cube_imag
        return jnp.stack([0.5 * (identity - sign_real), -0.5 * sign_imag])

    density = lax.map(purify, jnp.swapaxes(fock, 0, 1))
    mean_density = jnp.sum(density, axis=0) / K
    fragment_density = mean_density[:, slots[:, :, None], slots[:, None, :]]

    cell_ids = jnp.arange(K, dtype=jnp.int32)
    modded = (cell_ids[:, None] * cell_ids[None, :]) % K
    angle = modded.astype(jnp.float32) * (2.0 * math.pi / K)
    cos_table = jnp.cos(angle) / K
    sin_table = jnp.sin(angle) / K
    flat_real = density[:, 0].reshape(K, NORB * NORB)
    flat_imag = density[:, 1].reshape(K, NORB * NORB)
    high = lax.Precision.HIGHEST
    cell_real = jnp.dot(cos_table, flat_real, precision=high) - jnp.dot(sin_table, flat_imag, precision=high)
    cell_imag = jnp.dot(cos_table, flat_imag, precision=high) + jnp.dot(sin_table, flat_real, precision=high)
    density_cells = jnp.stack([cell_real.reshape(K, NORB, NORB), cell_imag.reshape(K, NORB, NORB)])
    return density_cells, fragment_density
```

```python
import functools
import math

import jax
import jax.numpy as jnp
import numpy as np
from jax import lax
from jax.experimental import pallas as pl
from jax.experimental.pallas import tpu as pltpu
from jax.sharding import PartitionSpec as P

ITERS = 2
N = 384
K = 256
F32 = jnp.float32
BF16 = jnp.bfloat16
MESH = pl.DeviceIdType.MESH


def split2(x):
    hi = x.astype(BF16)
    return hi, (x - hi.astype(F32)).astype(BF16)


def dot(a, b):
    return jnp.dot(a, b, preferred_element_type=F32)


def dot3(a_hi, a_lo, b_hi, b_lo):
    return dot(a_hi, b_hi) + (dot(a_hi, b_lo) + dot(a_lo, b_hi))


def contract(a, b, dims):
    return lax.dot_general(
        a, b, (dims, ((), ())), precision=lax.Precision.HIGHEST, preferred_element_type=F32
    )


def iota(shape, dim):
    return lax.broadcasted_iota(jnp.int32, shape, dim)


def remote(src, dst, send, recv, ka, orb):
    return pltpu.make_async_remote_copy(
        src_ref=src, dst_ref=dst, send_sem=send, recv_sem=recv, device_id=(ka, orb), device_id_type=MESH
    )


def wait_bytes(ref, sem):
    pltpu.make_async_copy(ref, ref, sem).wait()


def tile_of(ka, yh):
    g = ka // 36
    return (3 - 3 * g) * (1 - yh) + (1 + g) * yh, ka - 36 * g


def frag_device(o, rt):
    far = (o % 3 == 0).astype(jnp.int32)
    odd = o // 2
    h = rt * 2 + odd
    z = h % 8
    return z * 8 + (z + 1 + 3 * (h // 8)) % 8, 2 * far


def kernel(
    fock, pot, chem, bound, imp, imp4, pof, t_hi, t_lo,
    cells, frag,
    m_src, m_all, pot_all, u_ref, w_hi, w_lo, x_ref, d_tiles, k_buf, o_buf, d0_buf, f_out, f_in,
    s_fock, r_fock, s_pot, r_pot, s_k, r_k, s_o, r_o, s_d0, r_d0, s_f, r_f,
):
    ka = lax.axis_index("ka")
    orb = lax.axis_index("orb")
    z, x, yl = ka // 8, (ka // 2) % 4, ka % 2
    yh, core = orb // 2, orb % 2
    me = ka * 4 + orb

    m_src[...] = fock[0] + fock[1]
    for step in (2, 3, 1):
        to = (orb + step) % 4
        remote(pot, pot_all.at[orb], s_pot.at[step], r_pot.at[step], ka, to).start()
    for step in (2, 3, 1):
        to = (orb + step) % 4
        remote(m_src.at[to], m_all.at[orb], s_fock.at[step], r_fock.at[step], ka, to).start()
    pot_all[orb] = pot[...]
    m_all[orb] = m_src[orb]

    for step in (1, 2, 3):
        remote(pot, pot_all.at[(orb + 4 - step) % 4], s_pot.at[step], r_pot.at[step], ka, orb).wait_recv()
    slot_of = iota((N, 192), 0)
    col_of = iota((N, 192), 1)
    frag_of = slot_of // 48
    pot_of = jnp.zeros((N, 192), jnp.int32)
    for f in range(8):
        pot_of = jnp.where(frag_of == f, pof[f], pot_of)
    pick = ((col_of % 4 == pot_of) & (col_of // 4 == slot_of - 48 * frag_of)).astype(F32)
    stacked = contract(pick, pot_all[...].reshape(192, 48), ((1,), (0,)))
    spread = (iota((48, N), 1) % 48 == iota((48, N), 0)).astype(F32)
    wide = contract(stacked, spread, ((1,), (0,)))
    rows, cols = iota((N, N), 0), iota((N, N), 1)
    wide = jnp.where(rows // 48 == cols // 48, wide, 0.0)
    wide = 0.5 * (wide + wide.T)
    place = (rows == imp[...]).astype(F32)
    u_ref[...] = contract(contract(place, wide, ((1,), (0,))), place, ((1,), (1,)))

    for step in (1, 2, 3):
        remote(
            m_src.at[0], m_all.at[(orb + 4 - step) % 4], s_fock.at[step], r_fock.at[step], ka, orb
        ).wait_recv()
    m = m_all[...].reshape(N, N)
    mt = m.T
    scale = 1.0 / bound[0]
    eye = (rows == cols).astype(F32)
    x_ref[:, :N] = (0.5 * (m + mt) + u_ref[...] - chem[0] * eye) * scale
    x_ref[:, N:] = (0.5 * (m - mt)) * scale
    for step in range(ITERS):
        hi, lo = split2(x_ref[...])
        for part, w in ((hi, w_hi), (lo, w_lo)):
            w[:N, :N] = part[:, :N]
            w[:N, N:] = part[:, N:]
            w[N:, :N] = -part[:, N:]
            w[N:, N:] = part[:, :N]
        s = dot3(hi, lo, w_hi[...], w_lo[...])
        s_hi, s_lo = split2(s)
        c = dot3(s_hi, s_lo, w_hi[...], w_lo[...])
        x_ref[...] = 1.5 * x_ref[...] - 0.5 * c
    eye_half = 0.5 * eye
    for part in range(2):
        for cb in range(3):
            value = -0.5 * x_ref[:, part * N + cb * 128 : part * N + cb * 128 + 128]
            if part == 0:
                value = value + eye_half[:, cb * 128 : cb * 128 + 128]
            value = value.reshape(4, 12, 8, 128)
            for o in range(4):
                base = o * 36 + cb * 12
                d_tiles[base : base + 12, part] = value[o]

    own_o, own_j = tile_of(ka, yh)
    extra = (core == 0) & (ka == 9 * z)
    has_tile = (core == 1) | extra
    t_o = jnp.where(core == 1, own_o, 2 - 2 * yh + 0)
    t_o = jnp.where(core == 1, own_o, jnp.where(yh == 1, 0, 2))
    t_j = jnp.where(core == 1, own_j, 28 + z)

    def send_k(tile, to_ka, to_orb):
        remote(d_tiles.at[tile], k_buf.at[me], s_k, r_k, to_ka, to_orb).start()

    def spread_k(d, carry):
        to_z = (z + d % 8) % 8
        to_x = (x + (d // 8) % 4) % 4
        to_yl = (yl + (d // 32) % 2) % 2
        to_yh = (yh + d // 64) % 2
        to_ka = to_z * 8 + to_x * 2 + to_yl
        o, j = tile_of(to_ka, to_yh)

        @pl.when((d > 0) | (core == 0))
        def _():
            send_k(o * 36 + j, to_ka, to_yh * 2 + 1)

        return carry

    lax.fori_loop(0, 128, spread_k, 0)

    def spread_extra(d, carry):
        to_z = (z + d % 8) % 8
        to_yh = (yh + d // 8) % 2
        o = 2 - 2 * to_yh

        @pl.when((d > 0) | jnp.logical_not(extra))
        def _():
            send_k(o * 36 + 28 + to_z, 9 * to_z, to_yh * 2)

        return carry

    lax.fori_loop(0, 16, spread_extra, 0)

    row, cb = t_j % 12, t_j // 12

    @pl.when(has_tile)
    def _():
        k_buf[me] = d_tiles[t_o * 36 + t_j]
        wait_bytes(k_buf.at[pl.ds(0, K - 1)], r_k)
        k_rows = k_buf.reshape(K * 16, 128)
        o_rows = o_buf.reshape(2 * K * 8, 128)
        for pair in range(4):
            parts = []
            for s in (2 * pair, 2 * pair + 1):
                parts.append(
                    jnp.concatenate([k_rows[pl.ds(c * 8 + s, K, stride=16), :] for c in range(2)], axis=0)
                )
            v_hi, v_lo = split2(jnp.concatenate(parts, axis=1))
            res = dot3(t_hi[...], t_lo[...], v_hi, v_lo)
            for n, s in enumerate((2 * pair, 2 * pair + 1)):
                for c in range(2):
                    o_rows[pl.ds(c * K * 8 + s, K, stride=8), :] = res[c * K : c * K + K, n * 128 : n * 128 + 128]

        def send_d0(g, carry):
            to_ka, to_orb = frag_device(g % 4, g // 4)
            remote(o_buf.at[:, 0], d0_buf.at[t_o * 36 + t_j], s_d0, r_d0, to_ka, to_orb).start()
            return carry

        lax.fori_loop(0, 24, send_d0, 0)

        def send_o(d, carry):
            to_z = (z + d % 8) % 8
            to_x = (x + (d // 8) % 4) % 4
            to_yl = (yl + d // 32) % 2
            to_ka = to_z * 8 + to_x * 2 + to_yl
            remote(
                o_buf.at[:, pl.ds(4 * to_ka, 4)],
                cells.at[:, :, pl.ds(pl.multiple_of(8 * row, 8), 8), pl.ds(pl.multiple_of(128 * cb, 128), 128)],
                s_o, r_o, to_ka, t_o,
            ).start()
            return carry

        lax.fori_loop(0, 64, send_o, 0)

    turn = (ka % 8 + 8 - z) % 8
    makes = (core == 0) & ((turn == 1) | ((turn == 4) & (z < 4)))
    h = jnp.where(turn == 1, z, 8 + z)
    f_rt, f_odd = h // 2, h % 2
    f_o = jnp.where(yh == 1, 3 * f_odd, 1 + f_odd)

    @pl.when(makes)
    def _():
        wait_bytes(d0_buf, r_d0)
        chosen = (iota((N, 128), 0) == imp4[pl.ds(f_o, 1), :]).astype(F32)
        left = iota((48, 128), 1) < 48
        for part in range(2):
            picked = jnp.zeros((128, 128), F32)
            for cb in range(3):
                block = jnp.concatenate(
                    [d0_buf[o * 36 + cb * 12 : o * 36 + cb * 12 + 12, part].reshape(96, 128) for o in range(4)],
                    axis=0,
                )
                some = contract(chosen, block, ((0,), (0,)))
                picked = picked + contract(some, chosen[cb * 128 : cb * 128 + 128], ((1,), (0,)))
            f_out[part] = jnp.where(left, picked[:48], picked[48:96])

        def send_f(d, carry):
            to_ka = ((z + d % 8) % 8) * 8 + (ka + d // 8) % 8
            rows_at = pl.ds(pl.multiple_of(8 * f_rt, 8), 8)
            remote(f_out.at[:, rows_at], f_in.at[:, rows_at], s_f, r_f, to_ka, f_o).start()
            return carry

        lax.fori_loop(0, 64, send_f, 0)

    wait_bytes(f_in, r_f)
    for part in range(2):
        for f in range(2):
            frag[part, f] = f_in[part, :, 48 * f : 48 * f + 48]
    wait_bytes(cells, r_o)

    for step in (1, 2, 3):
        remote(pot, pot_all.at[0], s_pot.at[step], r_pot.at[step], ka, orb).wait_send()
        remote(m_src.at[0], m_all.at[0], s_fock.at[step], r_fock.at[step], ka, orb).wait_send()
    wait_bytes(d_tiles.at[pl.ds(0, 143)], s_k)

    @pl.when(jnp.logical_not(has_tile))
    def _():
        wait_bytes(d_tiles.at[0], s_k)

    @pl.when(has_tile)
    def _():
        wait_bytes(d_tiles.at[pl.ds(0, 24)], s_d0)
        wait_bytes(o_buf, s_o)

    @pl.when(makes)
    def _():
        wait_bytes(d_tiles.at[pl.ds(0, 64)], s_f)


def tables():
    grid = np.outer(np.arange(K), np.arange(K)) % K
    angle = grid * (2.0 * math.pi / K)
    c, s = np.cos(angle) / K, np.sin(angle) / K
    full = np.block([[c, -s], [s, c]]).astype(np.float32)
    hi = full.astype(jnp.bfloat16)
    lo = (full - hi.astype(np.float32)).astype(jnp.bfloat16)
    return hi, lo


def per_device(fock, potential, chem_potential, spectral_bound, impurity_orbitals, potential_of):
    t_hi, t_lo = tables()
    vmem = pl.BlockSpec(memory_space=pltpu.VMEM)
    smem = pl.BlockSpec(memory_space=pltpu.SMEM)
    dma = pltpu.SemaphoreType.DMA
    pot = potential.transpose(1, 0, 2).reshape(48, 48)
    imp4 = jnp.pad(impurity_orbitals.reshape(4, 96), ((0, 0), (0, 32)), constant_values=-1)
    return pl.pallas_call(
        kernel,
        out_shape=(
            jax.ShapeDtypeStruct((2, 4, 96, N), F32),
            jax.ShapeDtypeStruct((2, 2, 48, 48), F32),
        ),
        in_specs=[vmem, vmem, smem, smem, vmem, vmem, smem, vmem, vmem],
        out_specs=(vmem, vmem),
        scratch_shapes=[
            pltpu.VMEM((4, 96, N), F32),
            pltpu.VMEM((4, 96, N), F32),
            pltpu.VMEM((4, 48, 48), F32),
            pltpu.VMEM((N, N), F32),
            pltpu.VMEM((2 * N, 2 * N), BF16),
            pltpu.VMEM((2 * N, 2 * N), BF16),
            pltpu.VMEM((N, 2 * N), F32),
            pltpu.VMEM((144, 2, 8, 128), F32),
            pltpu.VMEM((K, 2, 8, 128), F32),
            pltpu.VMEM((2, K, 8, 128), F32),
            pltpu.VMEM((144, 2, 8, 128), F32),
            pltpu.VMEM((2, 48, 128), F32),
            pltpu.VMEM((2, 48, 128), F32),
            dma((4,)), dma((4,)), dma((4,)), dma((4,)),
            dma, dma, dma, dma, dma, dma, dma, dma,
        ],
        compiler_params=pltpu.CompilerParams(has_side_effects=True, vmem_limit_bytes=56 << 20),
        cost_estimate=pl.CostEstimate(flops=10**10, bytes_accessed=10**7, transcendentals=0),
    )(
        fock, pot, chem_potential, spectral_bound,
        impurity_orbitals.reshape(1, N), imp4, potential_of,
        jnp.asarray(t_hi), jnp.asarray(t_lo),
    )


def solution(mesh):
    return jax.shard_map(
        per_device,
        mesh=mesh,
        in_specs=(P(None, "ka", "orb", None), P(None, "orb", None), P(), P(), P(), P()),
        out_specs=(P(None, "ka", "orb", None), P(None, "orb", None, None)),
        check_vma=False,
    )
```

```python
import functools
import math

import jax
import jax.numpy as jnp
import numpy as np
from jax import lax
from jax.experimental import pallas as pl
from jax.experimental.pallas import tpu as pltpu
from jax.sharding import PartitionSpec as P

ITERS = 2
N = 384
K = 256
F32 = jnp.float32
BF16 = jnp.bfloat16
MESH = pl.DeviceIdType.MESH


def split2(x):
    hi = x.astype(BF16)
    return hi, (x - hi.astype(F32)).astype(BF16)


def dot(a, b):
    return jnp.dot(a, b, preferred_element_type=F32)


def dot3(a_hi, a_lo, b_hi, b_lo):
    return dot(a_hi, b_hi) + (dot(a_hi, b_lo) + dot(a_lo, b_hi))


def contract(a, b, dims):
    return lax.dot_general(
        a, b, (dims, ((), ())), precision=lax.Precision.HIGHEST, preferred_element_type=F32
    )


def iota(shape, dim):
    return lax.broadcasted_iota(jnp.int32, shape, dim)


def remote(src, dst, send, recv, ka, orb):
    return pltpu.make_async_remote_copy(
        src_ref=src, dst_ref=dst, send_sem=send, recv_sem=recv, device_id=(ka, orb), device_id_type=MESH
    )


def wait_bytes(ref, sem):
    pltpu.make_async_copy(ref, ref, sem).wait()


def tile_of(ka, yh):
    g = ka // 36
    return (3 - 3 * g) * (1 - yh) + (1 + g) * yh, ka - 36 * g


def frag_device(o, rt):
    far = (o % 3 == 0).astype(jnp.int32)
    odd = o // 2
    h = rt * 2 + odd
    z = h % 8
    return z * 8 + (z + 1 + 3 * (h // 8)) % 8, 2 * far


def gather_kernel(
    fock, pot, chem, bound, imp, pof, x_out, m_src, m_all, pot_all, u_ref, s_fock, r_fock, s_pot, r_pot
):
    ka = lax.axis_index("ka")
    orb = lax.axis_index("orb")
    barrier = pltpu.get_barrier_semaphore()
    for step in (1, 2, 3):
        pl.semaphore_signal(barrier, inc=1, device_id=(ka, (orb + step) % 4), device_id_type=MESH)
    m_src[...] = fock[0] + fock[1]
    pl.semaphore_wait(barrier, 3)
    for step in (2, 3, 1):
        to = (orb + step) % 4
        remote(pot, pot_all.at[orb], s_pot.at[step], r_pot.at[step], ka, to).start()
    for step in (2, 3, 1):
        to = (orb + step) % 4
        remote(m_src.at[to], m_all.at[orb], s_fock.at[step], r_fock.at[step], ka, to).start()
    pot_all[orb] = pot[...]
    m_all[orb] = m_src[orb]

    for step in (1, 2, 3):
        remote(pot, pot_all.at[(orb + 4 - step) % 4], s_pot.at[step], r_pot.at[step], ka, orb).wait_recv()
    slot_of = iota((N, 192), 0)
    col_of = iota((N, 192), 1)
    frag_of = slot_of // 48
    pot_of = jnp.zeros((N, 192), jnp.int32)
    for f in range(8):
        pot_of = jnp.where(frag_of == f, pof[f], pot_of)
    pick = ((col_of % 4 == pot_of) & (col_of // 4 == slot_of - 48 * frag_of)).astype(F32)
    stacked = contract(pick, pot_all[...].reshape(192, 48), ((1,), (0,)))
    spread = (iota((48, N), 1) % 48 == iota((48, N), 0)).astype(F32)
    wide = contract(stacked, spread, ((1,), (0,)))
    rows, cols = iota((N, N), 0), iota((N, N), 1)
    wide = jnp.where(rows // 48 == cols // 48, wide, 0.0)
    wide = 0.5 * (wide + wide.T)
    place = (rows == imp[...]).astype(F32)
    u_ref[...] = contract(contract(place, wide, ((1,), (0,))), place, ((1,), (1,)))

    for step in (1, 2, 3):
        remote(
            m_src.at[0], m_all.at[(orb + 4 - step) % 4], s_fock.at[step], r_fock.at[step], ka, orb
        ).wait_recv()
    m = m_all[...].reshape(N, N)
    mt = m.T
    scale = 1.0 / bound[0]
    eye = (rows == cols).astype(F32)
    x_out[:, :N] = (0.5 * (m + mt) + u_ref[...] - chem[0] * eye) * scale
    x_out[:, N:] = (0.5 * (m - mt)) * scale
    for step in (1, 2, 3):
        remote(pot, pot_all.at[0], s_pot.at[step], r_pot.at[step], ka, orb).wait_send()
        remote(m_src.at[0], m_all.at[0], s_fock.at[step], r_fock.at[step], ka, orb).wait_send()


def main_kernel(
    x_in, imp, t_hi, t_lo, cells, f_in,
    x_ref, w_hi, w_lo, d_tiles, k_buf, o_buf, d0_buf, f_out,
    entered, s_k, r_k, s_o, r_o, s_d0, r_d0, s_f, r_f,
):
    ka = lax.axis_index("ka")
    orb = lax.axis_index("orb")
    z, x, yl = ka // 8, (ka // 2) % 4, ka % 2
    yh, core = orb // 2, orb % 2
    me = ka * 4 + orb
    barrier = pltpu.get_barrier_semaphore()

    def greet(d, carry):
        plane = (ka + d // 4) % 8
        pl.semaphore_signal(barrier, inc=1, device_id=(8 * z + plane, (orb + d) % 4), device_id_type=MESH)
        return carry

    lax.fori_loop(1, 32, greet, 0)
    for step in range(1, 8):
        pl.semaphore_signal(barrier, inc=1, device_id=((ka + 8 * step) % 64, orb), device_id_type=MESH)

    x_ref[...] = x_in[...]
    rows, cols = iota((N, N), 0), iota((N, N), 1)
    eye = (rows == cols).astype(F32)
    for step in range(ITERS):
        hi, lo = split2(x_ref[...])
        for part, w in ((hi, w_hi), (lo, w_lo)):
            w[:N, :N] = part[:, :N]
            w[:N, N:] = part[:, N:]
            w[N:, :N] = -part[:, N:]
            w[N:, N:] = part[:, :N]
        s = dot3(hi, lo, w_hi[...], w_lo[...])
        s_hi, s_lo = split2(s)
        c = dot3(s_hi, s_lo, w_hi[...], w_lo[...])
        x_ref[...] = 1.5 * x_ref[...] - 0.5 * c
        if step == 0:
            pl.semaphore_wait(barrier, 38)
            for hop in range(1, 8):
                pl.semaphore_signal(entered, inc=1, device_id=((ka + 8 * hop) % 64, orb), device_id_type=MESH)
    eye_half = 0.5 * eye
    for part in range(2):
        for cb in range(3):
            value = -0.5 * x_ref[:, part * N + cb * 128 : part * N + cb * 128 + 128]
            if part == 0:
                value = value + eye_half[:, cb * 128 : cb * 128 + 128]
            value = value.reshape(4, 12, 8, 128)
            for o in range(4):
                base = o * 36 + cb * 12
                d_tiles[base : base + 12, part] = value[o]

    own_o, own_j = tile_of(ka, yh)
    extra = (core == 0) & (ka == 9 * z)
    has_tile = (core == 1) | extra
    t_o = jnp.where(core == 1, own_o, jnp.where(yh == 1, 0, 2))
    t_j = jnp.where(core == 1, own_j, 28 + z)

    pl.semaphore_wait(entered, 7)

    def send_k(tile, to_ka, to_orb):
        remote(d_tiles.at[tile], k_buf.at[me], s_k, r_k, to_ka, to_orb).start()

    def spread_k(d, carry):
        to_z = (z + d % 8) % 8
        to_x = (x + (d // 8) % 4) % 4
        to_yl = (yl + (d // 32) % 2) % 2
        to_yh = (yh + d // 64) % 2
        to_ka = to_z * 8 + to_x * 2 + to_yl
        o, j = tile_of(to_ka, to_yh)

        @pl.when((d > 0) | (core == 0))
        def _():
            send_k(o * 36 + j, to_ka, to_yh * 2 + 1)

        return carry

    lax.fori_loop(0, 128, spread_k, 0)

    def spread_extra(d, carry):
        to_z = (z + d % 8) % 8
        to_yh = (yh + d // 8) % 2
        o = 2 - 2 * to_yh

        @pl.when((d > 0) | jnp.logical_not(extra))
        def _():
            send_k(o * 36 + 28 + to_z, 9 * to_z, to_yh * 2)

        return carry

    lax.fori_loop(0, 16, spread_extra, 0)

    row, cb = t_j % 12, t_j // 12

    @pl.when(has_tile)
    def _():
        k_buf[me] = d_tiles[t_o * 36 + t_j]
        wait_bytes(k_buf.at[pl.ds(0, K - 1)], r_k)
        k_rows = k_buf.reshape(K * 16, 128)
        o_rows = o_buf.reshape(2 * K * 8, 128)
        for pair in range(4):
            parts = []
            for s in (2 * pair, 2 * pair + 1):
                parts.append(
                    jnp.concatenate([k_rows[pl.ds(c * 8 + s, K, stride=16), :] for c in range(2)], axis=0)
                )
            v_hi, v_lo = split2(jnp.concatenate(parts, axis=1))
            res = dot3(t_hi[...], t_lo[...], v_hi, v_lo)
            for n, s in enumerate((2 * pair, 2 * pair + 1)):
                for c in range(2):
                    o_rows[pl.ds(c * K * 8 + s, K, stride=8), :] = res[c * K : c * K + K, n * 128 : n * 128 + 128]

        def send_d0(g, carry):
            to_ka, to_orb = frag_device(g % 4, g // 4)
            remote(o_buf.at[:, 0], d0_buf.at[t_o * 36 + t_j], s_d0, r_d0, to_ka, to_orb).start()
            return carry

        lax.fori_loop(0, 24, send_d0, 0)

        def send_o(d, carry):
            to_z = (z + d % 8) % 8
            to_x = (x + (d // 8) % 4) % 4
            to_yl = (yl + d // 32) % 2
            to_ka = to_z * 8 + to_x * 2 + to_yl
            remote(
                o_buf.at[:, pl.ds(4 * to_ka, 4)],
                cells.at[:, :, pl.ds(pl.multiple_of(8 * row, 8), 8), pl.ds(pl.multiple_of(128 * cb, 128), 128)],
                s_o, r_o, to_ka, t_o,
            ).start()
            return carry

        lax.fori_loop(0, 64, send_o, 0)

    turn = (ka % 8 + 8 - z) % 8
    makes = (core == 0) & ((turn == 1) | ((turn == 4) & (z < 4)))
    h = jnp.where(turn == 1, z, 8 + z)
    f_rt, f_odd = h // 2, h % 2
    f_o = jnp.where(yh == 1, 3 * f_odd, 1 + f_odd)

    @pl.when(makes)
    def _():
        slots = [imp[:, 96 * o : 96 * o + 96] for o in range(4)]
        own_slots = slots[0]
        for o in range(1, 4):
            own_slots = jnp.where(f_o == o, slots[o], own_slots)
        own_slots = jnp.concatenate([own_slots, jnp.full((1, 32), -1, jnp.int32)], axis=1)
        wait_bytes(d0_buf, r_d0)
        chosen = (iota((N, 128), 0) == own_slots).astype(F32)
        left = iota((48, 128), 1) < 48
        for part in range(2):
            picked = jnp.zeros((128, 128), F32)
            for cb in range(3):
                block = jnp.concatenate(
                    [d0_buf[o * 36 + cb * 12 : o * 36 + cb * 12 + 12, part].reshape(96, 128) for o in range(4)],
                    axis=0,
                )
                some = contract(chosen, block, ((0,), (0,)))
                picked = picked + contract(some, chosen[cb * 128 : cb * 128 + 128], ((1,), (0,)))
            f_out[part] = jnp.where(left, picked[:48], picked[48:96])

        def send_f(d, carry):
            to_ka = ((z + d % 8) % 8) * 8 + (ka + d // 8) % 8
            rows_at = pl.ds(pl.multiple_of(8 * f_rt, 8), 8)
            remote(f_out.at[:, rows_at], f_in.at[:, rows_at], s_f, r_f, to_ka, f_o).start()
            return carry

        lax.fori_loop(0, 64, send_f, 0)

    wait_bytes(f_in, r_f)
    wait_bytes(cells, r_o)

    wait_bytes(d_tiles.at[pl.ds(0, 143)], s_k)

    @pl.when(jnp.logical_not(has_tile))
    def _():
        wait_bytes(d_tiles.at[0], s_k)

    @pl.when(has_tile)
    def _():
        wait_bytes(d_tiles.at[pl.ds(0, 24)], s_d0)
        wait_bytes(o_buf, s_o)

    @pl.when(makes)
    def _():
        wait_bytes(d_tiles.at[pl.ds(0, 64)], s_f)


def store_kernel(cells, f_in, out, frag, sem):
    stores = [pltpu.make_async_copy(cells.at[c], out.at[c], sem.at[c]) for c in range(2)]
    for store in stores:
        store.start()
    for part in range(2):
        for f in range(2):
            frag[part, f] = f_in[part, :, 48 * f : 48 * f + 48]
    for store in stores:
        store.wait()


def tables():
    grid = np.outer(np.arange(K), np.arange(K)) % K
    angle = grid * (2.0 * math.pi / K)
    c, s = np.cos(angle) / K, np.sin(angle) / K
    full = np.block([[c, -s], [s, c]]).astype(np.float32)
    hi = full.astype(jnp.bfloat16)
    lo = (full - hi.astype(np.float32)).astype(jnp.bfloat16)
    return hi, lo


def per_device(fock, potential, chem_potential, spectral_bound, impurity_orbitals, potential_of):
    t_hi, t_lo = tables()
    vmem = pl.BlockSpec(memory_space=pltpu.VMEM)
    smem = pl.BlockSpec(memory_space=pltpu.SMEM)
    anywhere = pl.BlockSpec(memory_space=pl.ANY)
    dma = pltpu.SemaphoreType.DMA
    pot = potential.transpose(1, 0, 2).reshape(48, 48)
    imp = impurity_orbitals.reshape(1, N)
    start = pl.pallas_call(
        gather_kernel,
        name="gather",
        out_shape=jax.ShapeDtypeStruct((N, 2 * N), F32),
        in_specs=[vmem, vmem, smem, smem, vmem, smem],
        out_specs=vmem,
        scratch_shapes=[
            pltpu.VMEM((4, 96, N), F32),
            pltpu.VMEM((4, 96, N), F32),
            pltpu.VMEM((4, 48, 48), F32),
            pltpu.VMEM((N, N), F32),
            dma((4,)), dma((4,)), dma((4,)), dma((4,)),
        ],
        compiler_params=pltpu.CompilerParams(
            has_side_effects=True, collective_id=0, vmem_limit_bytes=40 << 20
        ),
    )(fock, pot, chem_potential, spectral_bound, imp, potential_of)
    cells, f_in = pl.pallas_call(
        main_kernel,
        name="transform",
        out_shape=(
            jax.ShapeDtypeStruct((2, 4, 96, N), F32),
            jax.ShapeDtypeStruct((2, 48, 128), F32),
        ),
        in_specs=[vmem, vmem, vmem, vmem],
        out_specs=(vmem, vmem),
        scratch_shapes=[
            pltpu.VMEM((N, 2 * N), F32),
            pltpu.VMEM((2 * N, 2 * N), BF16),
            pltpu.VMEM((2 * N, 2 * N), BF16),
            pltpu.VMEM((144, 2, 8, 128), F32),
            pltpu.VMEM((K, 2, 8, 128), F32),
            pltpu.VMEM((2, K, 8, 128), F32),
            pltpu.VMEM((144, 2, 8, 128), F32),
            pltpu.VMEM((2, 48, 128), F32),
            pltpu.SemaphoreType.REGULAR,
            dma, dma, dma, dma, dma, dma, dma, dma,
        ],
        compiler_params=pltpu.CompilerParams(
            has_side_effects=True, collective_id=1, vmem_limit_bytes=48 << 20
        ),
    )(start, imp, jnp.asarray(t_hi), jnp.asarray(t_lo))
    return pl.pallas_call(
        store_kernel,
        name="store",
        out_shape=(
            jax.ShapeDtypeStruct((2, 4, 96, N), F32),
            jax.ShapeDtypeStruct((2, 2, 48, 48), F32),
        ),
        in_specs=[vmem, vmem],
        out_specs=(anywhere, vmem),
        scratch_shapes=[dma((2,))],
    )(cells, f_in)


def solution(mesh):
    return jax.shard_map(
        per_device,
        mesh=mesh,
        in_specs=(P(None, "ka", "orb", None), P(None, "orb", None), P(), P(), P(), P()),
        out_specs=(P(None, "ka", "orb", None), P(None, "orb", None, None)),
        check_vma=False,
    )
```

```python
import functools
import math

import jax
import jax.numpy as jnp
import numpy as np
from jax import lax
from jax.experimental import pallas as pl
from jax.experimental.pallas import tpu as pltpu
from jax.sharding import PartitionSpec as P

ITERS = 2
N = 384
K = 256
F32 = jnp.float32
BF16 = jnp.bfloat16
MESH = pl.DeviceIdType.MESH


def split2(x):
    hi = x.astype(BF16)
    return hi, (x - hi.astype(F32)).astype(BF16)


def dot(a, b):
    return jnp.dot(a, b, preferred_element_type=F32)


def dot3(a_hi, a_lo, b_hi, b_lo):
    return dot(a_hi, b_hi) + (dot(a_hi, b_lo) + dot(a_lo, b_hi))


def contract(a, b, dims):
    return lax.dot_general(
        a, b, (dims, ((), ())), precision=lax.Precision.HIGHEST, preferred_element_type=F32
    )


def iota(shape, dim):
    return lax.broadcasted_iota(jnp.int32, shape, dim)


def remote(src, dst, send, recv, ka, orb):
    return pltpu.make_async_remote_copy(
        src_ref=src, dst_ref=dst, send_sem=send, recv_sem=recv, device_id=(ka, orb), device_id_type=MESH
    )


def wait_bytes(ref, sem):
    pltpu.make_async_copy(ref, ref, sem).wait()


def tile_of(ka, yh):
    g = ka // 36
    return (3 - 3 * g) * (1 - yh) + (1 + g) * yh, ka - 36 * g


def far_then_near(i):
    odd = i % 2
    return (1 - odd) * ((4 + i // 2) % 8) + odd * (3 - i // 2)


def frag_device(g):
    o = g % 4
    return 8 * g + (g + 1) % 8, 2 - 2 * (((o + 1) // 2) % 2)


def gather_kernel(
    fock_hbm, pot_hbm, chem, bound, imp_hbm, pof_hbm, x_out,
    fock, pot, imp_flat, pof, m_src, m_all, pot_all, u_ref, s_in, s_fock, r_fock, s_pot, r_pot,
):
    ka = lax.axis_index("ka")
    orb = lax.axis_index("orb")
    barrier = pltpu.get_barrier_semaphore()
    for step in (1, 2, 3):
        pl.semaphore_signal(barrier, inc=1, device_id=(ka, (orb + step) % 4), device_id_type=MESH)
    loads = [
        pltpu.make_async_copy(source, target, s_in.at[n])
        for n, (source, target) in enumerate(
            ((fock_hbm, fock), (pot_hbm, pot), (imp_hbm, imp_flat), (pof_hbm, pof))
        )
    ]
    for load in loads:
        load.start()
    for load in loads:
        load.wait()
    m_src[...] = fock[0] + fock[1]
    pl.semaphore_wait(barrier, 3)
    for step in (2, 3, 1):
        to = (orb + step) % 4
        remote(pot, pot_all.at[orb], s_pot.at[step], r_pot.at[step], ka, to).start()
    for step in (2, 3, 1):
        to = (orb + step) % 4
        remote(m_src.at[to], m_all.at[orb], s_fock.at[step], r_fock.at[step], ka, to).start()
    pot_all[orb] = pot[...]
    m_all[orb] = m_src[orb]

    for step in (1, 2, 3):
        remote(pot, pot_all.at[(orb + 4 - step) % 4], s_pot.at[step], r_pot.at[step], ka, orb).wait_recv()
    slot_of = iota((N, 192), 0)
    col_of = iota((N, 192), 1)
    frag_of = slot_of // 48
    pot_of = jnp.zeros((N, 192), jnp.int32)
    for f in range(8):
        pot_of = jnp.where(frag_of == f, pof[f], pot_of)
    pick = ((col_of % 4 == pot_of) & (col_of // 4 == slot_of - 48 * frag_of)).astype(F32)
    stacked = contract(pick, pot_all[...].reshape(192, 48), ((1,), (0,)))
    spread = (iota((48, N), 1) % 48 == iota((48, N), 0)).astype(F32)
    wide = contract(stacked, spread, ((1,), (0,)))
    rows, cols = iota((N, N), 0), iota((N, N), 1)
    wide = jnp.where(rows // 48 == cols // 48, wide, 0.0)
    wide = 0.5 * (wide + wide.T)
    place = (rows == imp_flat[...].reshape(1, N)).astype(F32)
    u_ref[...] = contract(contract(place, wide, ((1,), (0,))), place, ((1,), (1,)))

    for step in (1, 2, 3):
        remote(
            m_src.at[0], m_all.at[(orb + 4 - step) % 4], s_fock.at[step], r_fock.at[step], ka, orb
        ).wait_recv()
    m = m_all[...].reshape(N, N)
    mt = m.T
    scale = 1.0 / bound[0]
    eye = (rows == cols).astype(F32)
    x_out[:, :N] = (0.5 * (m + mt) + u_ref[...] - chem[0] * eye) * scale
    x_out[:, N:] = (0.5 * (m - mt)) * scale
    for step in (1, 2, 3):
        remote(pot, pot_all.at[0], s_pot.at[step], r_pot.at[step], ka, orb).wait_send()
        remote(m_src.at[0], m_all.at[0], s_fock.at[step], r_fock.at[step], ka, orb).wait_send()


def main_kernel(
    x_in, imp_hbm, t_hi, t_lo, cells, f_in,
    imp_flat,
    x_ref, w_hi, w_lo, d_tiles, k_buf, o_buf, d0_buf, f_out,
    s_imp, entered, s_k, r_k, s_o, r_o, s_d0, r_d0, s_f, r_f,
):
    ka = lax.axis_index("ka")
    orb = lax.axis_index("orb")
    z, x, yl = ka // 8, (ka // 2) % 4, ka % 2
    yh, core = orb // 2, orb % 2
    me = ka * 4 + orb
    barrier = pltpu.get_barrier_semaphore()

    def greet(d, carry):
        plane = (ka + d // 4) % 8
        pl.semaphore_signal(barrier, inc=1, device_id=(8 * z + plane, (orb + d) % 4), device_id_type=MESH)
        return carry

    fetch = pltpu.make_async_copy(imp_hbm, imp_flat, s_imp)
    fetch.start()
    lax.fori_loop(1, 32, greet, 0)
    for step in range(1, 8):
        pl.semaphore_signal(barrier, inc=1, device_id=((ka + 8 * step) % 64, orb), device_id_type=MESH)

    x_ref[...] = x_in[...]
    rows, cols = iota((N, N), 0), iota((N, N), 1)
    eye = (rows == cols).astype(F32)
    for step in range(ITERS):
        hi, lo = split2(x_ref[...])
        for part, w in ((hi, w_hi), (lo, w_lo)):
            w[:N, :N] = part[:, :N]
            w[:N, N:] = part[:, N:]
            w[N:, :N] = -part[:, N:]
            w[N:, N:] = part[:, :N]
        s = dot3(hi, lo, w_hi[...], w_lo[...])
        s_hi, s_lo = split2(s)
        c = dot3(s_hi, s_lo, w_hi[...], w_lo[...])
        x_ref[...] = 1.5 * x_ref[...] - 0.5 * c
        if step == 0:
            fetch.wait()
            pl.semaphore_wait(barrier, 38)
            for hop in range(1, 8):
                pl.semaphore_signal(entered, inc=1, device_id=((ka + 8 * hop) % 64, orb), device_id_type=MESH)
    eye_half = 0.5 * eye
    for part in range(2):
        for cb in range(3):
            value = -0.5 * x_ref[:, part * N + cb * 128 : part * N + cb * 128 + 128]
            if part == 0:
                value = value + eye_half[:, cb * 128 : cb * 128 + 128]
            value = value.reshape(4, 12, 8, 128)
            for o in range(4):
                base = o * 36 + cb * 12
                d_tiles[base : base + 12, part] = value[o]

    own_o, own_j = tile_of(ka, yh)
    extra = (core == 0) & (ka == 9 * z)
    has_tile = (core == 1) | extra
    t_o = jnp.where(core == 1, own_o, jnp.where(yh == 1, 0, 2))
    t_j = jnp.where(core == 1, own_j, 28 + z)

    pl.semaphore_wait(entered, 7)

    def send_k(tile, to_ka, to_orb):
        remote(d_tiles.at[tile], k_buf.at[me], s_k, r_k, to_ka, to_orb).start()

    for half in range(2):

        def spread_k(d, carry, half=half):
            step_z = far_then_near(d % 8)
            to_z = (z + step_z) % 8
            to_x = (x + (d // 8) % 4) % 4
            to_yh = (yh + d // 32) % 2
            to_ka = to_z * 8 + to_x * 2 + half
            o, j = tile_of(to_ka, to_yh)

            @pl.when((d != 7) | (yl != half) | (core == 0))
            def _():
                send_k(o * 36 + j, to_ka, to_yh * 2 + 1)

            return carry

        lax.fori_loop(0, 64, spread_k, 0)

        def spread_extra(d, carry, half=half):
            to_z = 2 * ((z // 2 + d % 4) % 4) + half
            to_yh = (yh + d // 4) % 2
            o = 2 - 2 * to_yh

            @pl.when((d > 0) | (to_z != z) | jnp.logical_not(extra))
            def _():
                send_k(o * 36 + 28 + to_z, 9 * to_z, to_yh * 2)

            return carry

        lax.fori_loop(0, 8, spread_extra, 0)

    row, cb = t_j % 12, t_j // 12

    @pl.when(has_tile)
    def _():
        k_buf[me] = d_tiles[t_o * 36 + t_j]
        wait_bytes(k_buf.at[pl.ds(0, K - 1)], r_k)
        k_rows = k_buf.reshape(K * 16, 128)
        o_rows = o_buf.reshape(2 * K * 8, 128)
        for pair in range(4):
            parts = []
            for s in (2 * pair, 2 * pair + 1):
                parts.append(
                    jnp.concatenate([k_rows[pl.ds(c * 8 + s, K, stride=16), :] for c in range(2)], axis=0)
                )
            v_hi, v_lo = split2(jnp.concatenate(parts, axis=1))
            res = dot3(t_hi[...], t_lo[...], v_hi, v_lo)
            for n, s in enumerate((2 * pair, 2 * pair + 1)):
                for c in range(2):
                    o_rows[pl.ds(c * K * 8 + s, K, stride=8), :] = res[c * K : c * K + K, n * 128 : n * 128 + 128]

        def send_d0(g, carry):
            to_ka, to_orb = frag_device(g)
            remote(o_buf.at[:, 0], d0_buf.at[t_o * 36 + t_j], s_d0, r_d0, to_ka, to_orb).start()
            return carry

        lax.fori_loop(0, 8, send_d0, 0)

        def send_o(d, carry):
            to_z = (z + far_then_near(d % 8)) % 8
            to_x = (x + (d // 8) % 4) % 4
            to_yl = (yl + d // 32) % 2
            to_ka = to_z * 8 + to_x * 2 + to_yl
            remote(
                o_buf.at[:, pl.ds(4 * to_ka, 4)],
                cells.at[:, :, pl.ds(pl.multiple_of(8 * row, 8), 8), pl.ds(pl.multiple_of(128 * cb, 128), 128)],
                s_o, r_o, to_ka, t_o,
            ).start()
            return carry

        lax.fori_loop(0, 64, send_o, 0)

    f_o, f_half = z % 4, z // 4
    makes = (core == 0) & (ka % 8 == (z + 1) % 8) & (yh == 1 - ((f_o + 1) // 2) % 2)

    @pl.when(makes)
    def _():
        imp = imp_flat[...].reshape(1, N)
        slots = [imp[:, 96 * o : 96 * o + 96] for o in range(4)]
        own_slots = slots[0]
        for o in range(1, 4):
            own_slots = jnp.where(f_o == o, slots[o], own_slots)
        own_slots = jnp.concatenate([own_slots, jnp.full((1, 32), -1, jnp.int32)], axis=1)
        wait_bytes(d0_buf, r_d0)
        chosen = (iota((N, 128), 0) == own_slots).astype(F32)
        left = iota((48, 128), 1) < 48
        for part in range(2):
            picked = jnp.zeros((128, 128), F32)
            for cb in range(3):
                block = jnp.concatenate(
                    [d0_buf[o * 36 + cb * 12 : o * 36 + cb * 12 + 12, part].reshape(96, 128) for o in range(4)],
                    axis=0,
                )
                some = contract(chosen, block, ((0,), (0,)))
                picked = picked + contract(some, chosen[cb * 128 : cb * 128 + 128], ((1,), (0,)))
            f_out[part] = jnp.where(left, picked[:48], picked[48:96])

        def send_f(d, carry):
            to_ka = ((z + far_then_near(d % 8)) % 8) * 8 + (ka + d // 8) % 8
            rows_at = pl.ds(pl.multiple_of(24 * f_half, 8), 24)
            remote(f_out.at[:, rows_at], f_in.at[:, rows_at], s_f, r_f, to_ka, f_o).start()
            return carry

        lax.fori_loop(0, 64, send_f, 0)

    wait_bytes(f_in, r_f)
    wait_bytes(cells, r_o)

    wait_bytes(d_tiles.at[pl.ds(0, 143)], s_k)

    @pl.when(jnp.logical_not(has_tile))
    def _():
        wait_bytes(d_tiles.at[0], s_k)

    @pl.when(has_tile)
    def _():
        wait_bytes(d_tiles.at[pl.ds(0, 8)], s_d0)
        wait_bytes(o_buf, s_o)

    @pl.when(makes)
    def _():
        wait_bytes(k_buf.at[pl.ds(0, 192)], s_f)


def store_kernel(cells, f_in, out, frag, sem):
    stores = [pltpu.make_async_copy(cells.at[c], out.at[c], sem.at[c]) for c in range(2)]
    for store in stores:
        store.start()
    for part in range(2):
        for f in range(2):
            frag[part, f] = f_in[part, :, 48 * f : 48 * f + 48]
    for store in stores:
        store.wait()


def tables():
    grid = np.outer(np.arange(K), np.arange(K)) % K
    angle = grid * (2.0 * math.pi / K)
    c, s = np.cos(angle) / K, np.sin(angle) / K
    full = np.block([[c, -s], [s, c]]).astype(np.float32)
    hi = full.astype(jnp.bfloat16)
    lo = (full - hi.astype(np.float32)).astype(jnp.bfloat16)
    return hi, lo


def per_device(fock, potential, chem_potential, spectral_bound, impurity_orbitals, potential_of):
    t_hi, t_lo = tables()
    vmem = pl.BlockSpec(memory_space=pltpu.VMEM)
    smem = pl.BlockSpec(memory_space=pltpu.SMEM)
    hbm = pl.BlockSpec(memory_space=pltpu.HBM)
    dma = pltpu.SemaphoreType.DMA
    pot = potential.transpose(1, 0, 2).reshape(48, 48)
    imp = pltpu.with_memory_space_constraint(impurity_orbitals, pltpu.HBM)
    start = pl.pallas_call(
        gather_kernel,
        name="gather",
        out_shape=jax.ShapeDtypeStruct((N, 2 * N), F32),
        in_specs=[hbm, hbm, smem, smem, hbm, hbm],
        out_specs=vmem,
        scratch_shapes=[
            pltpu.VMEM((2, 4, 96, N), F32),
            pltpu.VMEM((48, 48), F32),
            pltpu.VMEM((N,), jnp.int32),
            pltpu.SMEM((8,), jnp.int32),
            pltpu.VMEM((4, 96, N), F32),
            pltpu.VMEM((4, 96, N), F32),
            pltpu.VMEM((4, 48, 48), F32),
            pltpu.VMEM((N, N), F32),
            dma((4,)), dma((4,)), dma((4,)), dma((4,)), dma((4,)),
        ],
        compiler_params=pltpu.CompilerParams(
            has_side_effects=True, collective_id=0, vmem_limit_bytes=40 << 20
        ),
    )(
        pltpu.with_memory_space_constraint(fock, pltpu.HBM),
        pltpu.with_memory_space_constraint(pot, pltpu.HBM),
        chem_potential,
        spectral_bound,
        imp,
        pltpu.with_memory_space_constraint(potential_of, pltpu.HBM),
    )
    cells, f_in = pl.pallas_call(
        main_kernel,
        name="transform",
        out_shape=(
            jax.ShapeDtypeStruct((2, 4, 96, N), F32),
            jax.ShapeDtypeStruct((2, 48, 128), F32),
        ),
        in_specs=[vmem, hbm, vmem, vmem],
        out_specs=(vmem, vmem),
        scratch_shapes=[
            pltpu.VMEM((N,), jnp.int32),
            pltpu.VMEM((N, 2 * N), F32),
            pltpu.VMEM((2 * N, 2 * N), BF16),
            pltpu.VMEM((2 * N, 2 * N), BF16),
            pltpu.VMEM((144, 2, 8, 128), F32),
            pltpu.VMEM((K, 2, 8, 128), F32),
            pltpu.VMEM((2, K, 8, 128), F32),
            pltpu.VMEM((144, 2, 8, 128), F32),
            pltpu.VMEM((2, 48, 128), F32),
            dma,
            pltpu.SemaphoreType.REGULAR,
            dma, dma, dma, dma, dma, dma, dma, dma,
        ],
        compiler_params=pltpu.CompilerParams(
            has_side_effects=True, collective_id=1, vmem_limit_bytes=48 << 20
        ),
    )(start, imp, jnp.asarray(t_hi), jnp.asarray(t_lo))
    return pl.pallas_call(
        store_kernel,
        name="store",
        out_shape=(
            jax.ShapeDtypeStruct((2, 4, 96, N), F32),
            jax.ShapeDtypeStruct((2, 2, 48, 48), F32),
        ),
        in_specs=[vmem, vmem],
        out_specs=(hbm, vmem),
        scratch_shapes=[dma((2,))],
        compiler_params=pltpu.CompilerParams(vmem_limit_bytes=4 << 20),
    )(cells, f_in)


def solution(mesh):
    return jax.shard_map(
        per_device,
        mesh=mesh,
        in_specs=(P(None, "ka", "orb", None), P(None, "orb", None), P(), P(), P(), P()),
        out_specs=(P(None, "ka", "orb", None), P(None, "orb", None, None)),
        check_vma=False,
    )
```

```python
import functools
import math

import jax
import jax.numpy as jnp
import numpy as np
from jax import lax
from jax.experimental import pallas as pl
from jax.experimental.pallas import tpu as pltpu
from jax.sharding import PartitionSpec as P

ITERS = 2
N = 384
K = 256
F32 = jnp.float32
BF16 = jnp.bfloat16
MESH = pl.DeviceIdType.MESH


def split2(x):
    hi = x.astype(BF16)
    return hi, (x - hi.astype(F32)).astype(BF16)


def dot(a, b):
    return jnp.dot(a, b, preferred_element_type=F32)


def dot3(a_hi, a_lo, b_hi, b_lo):
    return dot(a_hi, b_hi) + (dot(a_hi, b_lo) + dot(a_lo, b_hi))


def contract(a, b, dims):
    return lax.dot_general(
        a, b, (dims, ((), ())), precision=lax.Precision.HIGHEST, preferred_element_type=F32
    )


def iota(shape, dim):
    return lax.broadcasted_iota(jnp.int32, shape, dim)


def remote(src, dst, send, recv, ka, orb):
    return pltpu.make_async_remote_copy(
        src_ref=src, dst_ref=dst, send_sem=send, recv_sem=recv, device_id=(ka, orb), device_id_type=MESH
    )


def wait_bytes(ref, sem):
    pltpu.make_async_copy(ref, ref, sem).wait()


PAIRS = ((0, 1), (0, 2), (0, 3), (1, 2), (1, 3), (2, 3), (0, 0), (1, 1), (2, 2), (3, 3))
TILES = 9 * len(PAIRS)


def pack(block):
    a, b, c, d = (block[24 * n : 24 * n + 24] for n in range(4))
    return jnp.concatenate(
        [
            jnp.concatenate([a, b[:, :32]], axis=1),
            jnp.concatenate([b[:, 32:], c[:, :64]], axis=1),
            jnp.concatenate([c[:, 64:], d], axis=1),
        ],
        axis=0,
    )


def unpack(packed):
    p, q, r = (packed[24 * n : 24 * n + 24] for n in range(3))
    return jnp.concatenate(
        [
            p[:, :96],
            jnp.concatenate([p[:, 96:], q[:, :64]], axis=1),
            jnp.concatenate([q[:, 64:], r[:, :32]], axis=1),
            r[:, 32:],
        ],
        axis=0,
    )


def blocks_of(pair):
    late, last = (pair >= 3).astype(jnp.int32), (pair >= 5).astype(jnp.int32)
    diagonal = pair >= 6
    return (
        jnp.where(diagonal, pair - 6, late + last),
        jnp.where(diagonal, pair - 6, pair + 1 - 2 * late - last),
    )


def tile_at(z, x, yl, yh):
    column = x * 4 + yh * 2 + yl
    turn = (z + 16 - column) % 8
    tile = (turn - turn // 4) * 16 + column
    return tile, (turn % 4 != 3) & (tile < TILES)


def far_then_near(i):
    odd = i % 2
    return (1 - odd) * ((4 + i // 2) % 8) + odd * (3 - i // 2)


def frag_device(g):
    o = g % 4
    return 8 * g + (g + 1) % 8, 2 - 2 * (((o + 1) // 2) % 2)


def gather_kernel(
    fock_hbm, pot_hbm, chem, bound, imp_hbm, pof_hbm, x_out,
    fock, pot, imp_flat, pof, m_src, m_all, pot_all, u_ref, s_in, s_fock, r_fock, s_pot, r_pot,
):
    ka = lax.axis_index("ka")
    orb = lax.axis_index("orb")
    barrier = pltpu.get_barrier_semaphore()
    for step in (1, 2, 3):
        pl.semaphore_signal(barrier, inc=1, device_id=(ka, (orb + step) % 4), device_id_type=MESH)
    loads = [
        pltpu.make_async_copy(source, target, s_in.at[n])
        for n, (source, target) in enumerate(
            ((fock_hbm, fock), (pot_hbm, pot), (imp_hbm, imp_flat), (pof_hbm, pof))
        )
    ]
    for load in loads:
        load.start()
    for load in loads:
        load.wait()
    m_src[...] = fock[0] + fock[1]
    pl.semaphore_wait(barrier, 3)
    for step in (2, 3, 1):
        to = (orb + step) % 4
        remote(pot, pot_all.at[orb], s_pot.at[step], r_pot.at[step], ka, to).start()
    for step in (2, 3, 1):
        to = (orb + step) % 4
        remote(m_src.at[to], m_all.at[orb], s_fock.at[step], r_fock.at[step], ka, to).start()
    pot_all[orb] = pot[...]
    m_all[orb] = m_src[orb]

    for step in (1, 2, 3):
        remote(pot, pot_all.at[(orb + 4 - step) % 4], s_pot.at[step], r_pot.at[step], ka, orb).wait_recv()
    slot_of = iota((N, 192), 0)
    col_of = iota((N, 192), 1)
    frag_of = slot_of // 48
    pot_of = jnp.zeros((N, 192), jnp.int32)
    for f in range(8):
        pot_of = jnp.where(frag_of == f, pof[f], pot_of)
    pick = ((col_of % 4 == pot_of) & (col_of // 4 == slot_of - 48 * frag_of)).astype(F32)
    stacked = contract(pick, pot_all[...].reshape(192, 48), ((1,), (0,)))
    spread = (iota((48, N), 1) % 48 == iota((48, N), 0)).astype(F32)
    wide = contract(stacked, spread, ((1,), (0,)))
    rows, cols = iota((N, N), 0), iota((N, N), 1)
    wide = jnp.where(rows // 48 == cols // 48, wide, 0.0)
    wide = 0.5 * (wide + wide.T)
    place = (rows == imp_flat[...].reshape(1, N)).astype(F32)
    u_ref[...] = contract(contract(place, wide, ((1,), (0,))), place, ((1,), (1,)))

    for step in (1, 2, 3):
        remote(
            m_src.at[0], m_all.at[(orb + 4 - step) % 4], s_fock.at[step], r_fock.at[step], ka, orb
        ).wait_recv()
    m = m_all[...].reshape(N, N)
    mt = m.T
    scale = 1.0 / bound[0]
    eye = (rows == cols).astype(F32)
    x_out[:, :N] = (0.5 * (m + mt) + u_ref[...] - chem[0] * eye) * scale
    x_out[:, N:] = (0.5 * (m - mt)) * scale
    for step in (1, 2, 3):
        remote(pot, pot_all.at[0], s_pot.at[step], r_pot.at[step], ka, orb).wait_send()
        remote(m_src.at[0], m_all.at[0], s_fock.at[step], r_fock.at[step], ka, orb).wait_send()


def main_kernel(
    x_in, imp_hbm, t_hi, t_lo, landing, f_in,
    imp_flat,
    x_ref, w_hi, w_lo, d_tiles, k_buf, o_buf, d0_buf, full, f_out,
    s_imp, entered, s_k, r_k, s_o, r_o, s_d0, r_d0, s_f, r_f,
):
    ka = lax.axis_index("ka")
    orb = lax.axis_index("orb")
    z, x, yl = ka // 8, (ka // 2) % 4, ka % 2
    yh, core = orb // 2, orb % 2
    me = ka * 4 + orb
    barrier = pltpu.get_barrier_semaphore()

    def greet(d, carry):
        plane = (ka + d // 4) % 8
        pl.semaphore_signal(barrier, inc=1, device_id=(8 * z + plane, (orb + d) % 4), device_id_type=MESH)
        return carry

    fetch = pltpu.make_async_copy(imp_hbm, imp_flat, s_imp)
    fetch.start()
    lax.fori_loop(1, 32, greet, 0)
    for step in range(1, 8):
        pl.semaphore_signal(barrier, inc=1, device_id=((ka + 8 * step) % 64, orb), device_id_type=MESH)

    x_ref[...] = x_in[...]
    rows, cols = iota((N, N), 0), iota((N, N), 1)
    eye = (rows == cols).astype(F32)
    for step in range(ITERS):
        hi, lo = split2(x_ref[...])
        for part, w in ((hi, w_hi), (lo, w_lo)):
            w[:N, :N] = part[:, :N]
            w[:N, N:] = part[:, N:]
            w[N:, :N] = -part[:, N:]
            w[N:, N:] = part[:, :N]
        s = dot3(hi, lo, w_hi[...], w_lo[...])
        s_hi, s_lo = split2(s)
        c = dot3(s_hi, s_lo, w_hi[...], w_lo[...])
        x_ref[...] = 1.5 * x_ref[...] - 0.5 * c
        if step == 0:
            fetch.wait()
            pl.semaphore_wait(barrier, 38)
            for hop in range(1, 8):
                pl.semaphore_signal(entered, inc=1, device_id=((ka + 8 * hop) % 64, orb), device_id_type=MESH)
    for part in range(2):
        value = -0.5 * x_ref[:, part * N : part * N + N]
        if part == 0:
            value = value + 0.5 * eye
        for n, (o, p) in enumerate(PAIRS):
            packed = pack(value[96 * o : 96 * o + 96, 96 * p : 96 * p + 96])
            d_tiles[9 * n : 9 * n + 9, part] = packed.reshape(9, 8, 128)

    own_tile, chip_has = tile_at(z, x, yl, yh)
    has_tile = (core == 1) & chip_has
    pl.semaphore_wait(entered, 7)

    def spread_k(d, carry):
        to_z = (z + far_then_near(d % 8)) % 8
        to_x = (x + (d // 8) % 4) % 4
        to_yl = (yl + (d // 32) % 2) % 2
        to_yh = (yh + d // 64) % 2
        tile, there = tile_at(to_z, to_x, to_yl, to_yh)

        @pl.when(there & ((d != 7) | (core == 0)))
        def _():
            to_ka = to_z * 8 + to_x * 2 + to_yl
            remote(d_tiles.at[tile], k_buf.at[me], s_k, r_k, to_ka, to_yh * 2 + 1).start()

        return carry

    lax.fori_loop(0, 128, spread_k, 0)
    t_o, t_p = blocks_of(own_tile // 9)
    t_m = own_tile % 9
    mirrored = t_o != t_p
    to_self = (t_o == orb) | (t_p == orb)

    @pl.when(has_tile)
    def _():
        k_buf[me] = d_tiles[own_tile]
        wait_bytes(k_buf.at[pl.ds(0, K - 1)], r_k)
        k_rows = k_buf.reshape(K * 16, 128)
        o_rows = o_buf.reshape(4 * K * 8, 128)
        for s in range(8):
            both = [k_rows[pl.ds(c * 8 + s, K, stride=16), :] for c in range(2)]
            v_hi, v_lo = split2(jnp.concatenate(both, axis=1))
            res = dot3(t_hi[...], t_lo[...], v_hi, v_lo)
            cos_re, cos_im = res[:K, :128], res[:K, 128:]
            sin_re, sin_im = res[K:, :128], res[K:, 128:]
            o_rows[pl.ds(s, K, stride=8), :] = cos_re - sin_im
            o_rows[pl.ds(K * 8 + s, K, stride=8), :] = cos_im + sin_re
            o_rows[pl.ds(2 * K * 8 + s, K, stride=8), :] = cos_re + sin_im
            o_rows[pl.ds(3 * K * 8 + s, K, stride=8), :] = sin_re - cos_im

        def send_d0(g, carry):
            to_ka, to_orb = frag_device(g)
            remote(o_buf.at[pl.ds(0, 2), 0], d0_buf.at[own_tile], s_d0, r_d0, to_ka, to_orb).start()
            return carry

        lax.fori_loop(0, 8, send_d0, 0)

        def send_o(d, carry):
            to_z = (z + far_then_near(d % 8)) % 8
            to_x = (x + (d // 8) % 4) % 4
            to_yl = (yl + d // 32) % 2
            to_ka = to_z * 8 + to_x * 2 + to_yl
            cells_at = pl.ds(4 * to_ka, 4)

            @pl.when((d != 7) | (t_o != orb))
            def _():
                remote(o_buf.at[pl.ds(0, 2), cells_at], landing.at[t_p * 9 + t_m], s_o, r_o, to_ka, t_o).start()

            @pl.when(mirrored & ((d != 7) | (t_p != orb)))
            def _():
                remote(o_buf.at[pl.ds(2, 2), cells_at], landing.at[t_o * 9 + t_m], s_o, r_o, to_ka, t_p).start()

            return carry

        lax.fori_loop(0, 64, send_o, 0)

        @pl.when(t_o == orb)
        def _():
            landing[t_p * 9 + t_m] = o_buf[:2, pl.ds(4 * ka, 4)]

        @pl.when(mirrored & (t_p == orb))
        def _():
            landing[t_o * 9 + t_m] = o_buf[2:, pl.ds(4 * ka, 4)]

    f_o, f_half = z % 4, z // 4
    makes = (core == 0) & (ka % 8 == (z + 1) % 8) & (yh == 1 - ((f_o + 1) // 2) % 2)

    @pl.when(makes)
    def _():
        imp = imp_flat[...].reshape(1, N)
        slots = [imp[:, 96 * o : 96 * o + 96] for o in range(4)]
        own_slots = slots[0]
        for o in range(1, 4):
            own_slots = jnp.where(f_o == o, slots[o], own_slots)
        own_slots = jnp.concatenate([own_slots, jnp.full((1, 32), -1, jnp.int32)], axis=1)
        wait_bytes(d0_buf, r_d0)
        chosen = (iota((N, 128), 0) == own_slots).astype(F32)
        left = iota((48, 128), 1) < 48
        for part in range(2):
            for n, (o, p) in enumerate(PAIRS):
                block = unpack(d0_buf[9 * n : 9 * n + 9, part].reshape(72, 128))
                full[96 * o : 96 * o + 96, 96 * p : 96 * p + 96] = block
                if o != p:
                    full[96 * p : 96 * p + 96, 96 * o : 96 * o + 96] = block.T if part == 0 else -block.T
            picked = contract(contract(chosen, full[...], ((0,), (0,))), chosen, ((1,), (0,)))
            f_out[part] = jnp.where(left, picked[:48], picked[48:96])

        def send_f(d, carry):
            to_ka = ((z + far_then_near(d % 8)) % 8) * 8 + (ka + d // 8) % 8
            rows_at = pl.ds(pl.multiple_of(24 * f_half, 8), 24)
            remote(f_out.at[:, rows_at], f_in.at[:, rows_at], s_f, r_f, to_ka, f_o).start()
            return carry

        lax.fori_loop(0, 64, send_f, 0)

    wait_bytes(f_in, r_f)
    keeps = has_tile & to_self

    @pl.when(keeps)
    def _():
        wait_bytes(landing.at[pl.ds(0, 35)], r_o)

    @pl.when(jnp.logical_not(keeps))
    def _():
        wait_bytes(landing, r_o)

    @pl.when(has_tile)
    def _():
        wait_bytes(d_tiles.at[pl.ds(0, TILES - 1)], s_k)
        wait_bytes(d_tiles.at[pl.ds(0, 8)], s_d0)

    @pl.when(jnp.logical_not(has_tile))
    def _():
        wait_bytes(d_tiles, s_k)

    sides = ((mirrored, o_buf, K - 2), (jnp.logical_not(mirrored), o_buf.at[pl.ds(0, 2)], K - 4))
    for side, sent, fewer in sides:

        @pl.when(has_tile & side & to_self)
        def _(sent=sent, fewer=fewer):
            wait_bytes(sent.at[:, pl.ds(0, fewer)], s_o)

        @pl.when(has_tile & side & jnp.logical_not(to_self))
        def _(sent=sent):
            wait_bytes(sent, s_o)

    @pl.when(makes)
    def _():
        wait_bytes(k_buf.at[pl.ds(0, 192)], s_f)


def store_kernel(landing, f_in, out, frag, buf, sem):
    own = lax.axis_index("orb")
    stores = []
    for c in range(2):
        for r in range(4):
            for q in range(4):
                block = unpack(landing[9 * q : 9 * q + 9, c, r].reshape(72, 128))

                @pl.when(own <= q)
                def _(block=block, c=c, r=r, q=q):
                    buf[c, r, :, 96 * q : 96 * q + 96] = block

                @pl.when(own > q)
                def _(block=block, c=c, r=r, q=q):
                    buf[c, r, :, 96 * q : 96 * q + 96] = block.T

            stores.append(pltpu.make_async_copy(buf.at[c, r], out.at[c, r], sem.at[c, r]))
            stores[-1].start()
    for part in range(2):
        for f in range(2):
            frag[part, f] = f_in[part, :, 48 * f : 48 * f + 48]
    for store in stores:
        store.wait()


def tables():
    grid = np.outer(np.arange(K), np.arange(K)) % K
    angle = grid * (2.0 * math.pi / K)
    c, s = np.cos(angle) / K, np.sin(angle) / K
    full = np.concatenate([c, s]).astype(np.float32)
    hi = full.astype(jnp.bfloat16)
    lo = (full - hi.astype(np.float32)).astype(jnp.bfloat16)
    return hi, lo


def per_device(fock, potential, chem_potential, spectral_bound, impurity_orbitals, potential_of):
    t_hi, t_lo = tables()
    vmem = pl.BlockSpec(memory_space=pltpu.VMEM)
    smem = pl.BlockSpec(memory_space=pltpu.SMEM)
    hbm = pl.BlockSpec(memory_space=pltpu.HBM)
    dma = pltpu.SemaphoreType.DMA
    pot = potential.transpose(1, 0, 2).reshape(48, 48)
    imp = pltpu.with_memory_space_constraint(impurity_orbitals, pltpu.HBM)
    start = pl.pallas_call(
        gather_kernel,
        name="gather",
        out_shape=jax.ShapeDtypeStruct((N, 2 * N), F32),
        in_specs=[hbm, hbm, smem, smem, hbm, hbm],
        out_specs=vmem,
        scratch_shapes=[
            pltpu.VMEM((2, 4, 96, N), F32),
            pltpu.VMEM((48, 48), F32),
            pltpu.VMEM((N,), jnp.int32),
            pltpu.SMEM((8,), jnp.int32),
            pltpu.VMEM((4, 96, N), F32),
            pltpu.VMEM((4, 96, N), F32),
            pltpu.VMEM((4, 48, 48), F32),
            pltpu.VMEM((N, N), F32),
            dma((4,)), dma((4,)), dma((4,)), dma((4,)), dma((4,)),
        ],
        compiler_params=pltpu.CompilerParams(
            has_side_effects=True, collective_id=0, vmem_limit_bytes=40 << 20
        ),
    )(
        pltpu.with_memory_space_constraint(fock, pltpu.HBM),
        pltpu.with_memory_space_constraint(pot, pltpu.HBM),
        chem_potential,
        spectral_bound,
        imp,
        pltpu.with_memory_space_constraint(potential_of, pltpu.HBM),
    )
    landing, f_in = pl.pallas_call(
        main_kernel,
        name="transform",
        out_shape=(
            jax.ShapeDtypeStruct((36, 2, 4, 8, 128), F32),
            jax.ShapeDtypeStruct((2, 48, 128), F32),
        ),
        in_specs=[vmem, hbm, vmem, vmem],
        out_specs=(vmem, vmem),
        scratch_shapes=[
            pltpu.VMEM((N,), jnp.int32),
            pltpu.VMEM((N, 2 * N), F32),
            pltpu.VMEM((2 * N, 2 * N), BF16),
            pltpu.VMEM((2 * N, 2 * N), BF16),
            pltpu.VMEM((TILES, 2, 8, 128), F32),
            pltpu.VMEM((K, 2, 8, 128), F32),
            pltpu.VMEM((4, K, 8, 128), F32),
            pltpu.VMEM((TILES, 2, 8, 128), F32),
            pltpu.VMEM((N, N), F32),
            pltpu.VMEM((2, 48, 128), F32),
            dma,
            pltpu.SemaphoreType.REGULAR,
            dma, dma, dma, dma, dma, dma, dma, dma,
        ],
        compiler_params=pltpu.CompilerParams(
            has_side_effects=True, collective_id=1, vmem_limit_bytes=48 << 20
        ),
    )(start, imp, jnp.asarray(t_hi), jnp.asarray(t_lo))
    return pl.pallas_call(
        store_kernel,
        name="store",
        out_shape=(
            jax.ShapeDtypeStruct((2, 4, 96, N), F32),
            jax.ShapeDtypeStruct((2, 2, 48, 48), F32),
        ),
        in_specs=[vmem, vmem],
        out_specs=(hbm, vmem),
        scratch_shapes=[pltpu.VMEM((2, 4, 96, N), F32), dma((2, 4))],
        compiler_params=pltpu.CompilerParams(vmem_limit_bytes=8 << 20),
    )(landing, f_in)


def solution(mesh):
    return jax.shard_map(
        per_device,
        mesh=mesh,
        in_specs=(P(None, "ka", "orb", None), P(None, "orb", None), P(), P(), P(), P()),
        out_specs=(P(None, "ka", "orb", None), P(None, "orb", None, None)),
        check_vma=False,
    )
```

```python
import functools
import math

import jax
import jax.numpy as jnp
import numpy as np
from jax import lax
from jax.experimental import pallas as pl
from jax.experimental.pallas import tpu as pltpu
from jax.sharding import PartitionSpec as P

ITERS = 2
N = 384
K = 256
F32 = jnp.float32
BF16 = jnp.bfloat16
MESH = pl.DeviceIdType.MESH


def split2(x):
    hi = x.astype(BF16)
    return hi, (x - hi.astype(F32)).astype(BF16)


def dot(a, b):
    return jnp.dot(a, b, preferred_element_type=F32)


def dot3(a_hi, a_lo, b_hi, b_lo):
    return dot(a_hi, b_hi) + (dot(a_hi, b_lo) + dot(a_lo, b_hi))


def contract(a, b, dims):
    return lax.dot_general(
        a, b, (dims, ((), ())), precision=lax.Precision.HIGHEST, preferred_element_type=F32
    )


def iota(shape, dim):
    return lax.broadcasted_iota(jnp.int32, shape, dim)


def remote(src, dst, send, recv, ka, orb):
    return pltpu.make_async_remote_copy(
        src_ref=src, dst_ref=dst, send_sem=send, recv_sem=recv, device_id=(ka, orb), device_id_type=MESH
    )


def wait_bytes(ref, sem):
    pltpu.make_async_copy(ref, ref, sem).wait()


PAIRS = ((0, 1), (0, 2), (0, 3), (1, 2), (1, 3), (2, 3), (0, 0), (1, 1), (2, 2), (3, 3))
TILES = 18 * len(PAIRS)


def pack(block):
    a, b, c, d = (block[24 * n : 24 * n + 24] for n in range(4))
    return jnp.concatenate(
        [
            jnp.concatenate([a, b[:, :32]], axis=1),
            jnp.concatenate([b[:, 32:], c[:, :64]], axis=1),
            jnp.concatenate([c[:, 64:], d], axis=1),
        ],
        axis=0,
    )


def unpack(packed):
    p, q, r = (packed[24 * n : 24 * n + 24] for n in range(3))
    return jnp.concatenate(
        [
            p[:, :96],
            jnp.concatenate([p[:, 96:], q[:, :64]], axis=1),
            jnp.concatenate([q[:, 64:], r[:, :32]], axis=1),
            r[:, 32:],
        ],
        axis=0,
    )


def blocks_of(pair):
    late, last = (pair >= 3).astype(jnp.int32), (pair >= 5).astype(jnp.int32)
    diagonal = pair >= 6
    return (
        jnp.where(diagonal, pair - 6, late + last),
        jnp.where(diagonal, pair - 6, pair + 1 - 2 * late - last),
    )


def column_of(x, yl, yh):
    return x * 4 + yh * 2 + yl


def tiles_at(z, column):
    turn = (z + 16 - column) % 8
    late = (turn == 6) & (column >= 12)
    first = jnp.where(turn == 7, 124 + column, jnp.where(late, 164 + column, turn * 16 + column))
    second = jnp.where(turn == 7, 108, jnp.where(turn == 1, 140, jnp.where(turn == 5, 156, 160))) + column
    return first, second, (turn == 7) | (turn == 1) | (turn == 5) | late


def far_then_near(i):
    odd = i % 2
    return (1 - odd) * ((4 + i // 2) % 8) + odd * (3 - i // 2)


def frag_device(g):
    column = (g + 6) % 8
    return 8 * g + 2 * (column // 4) + column % 2, 2 * ((column // 2) % 2)


def gather_kernel(
    fock_hbm, pot_hbm, chem, bound, imp_hbm, pof_hbm, x_out,
    fock, pot, imp_flat, pof, m_src, m_all, pot_all, u_ref, s_in, s_fock, r_fock, s_pot, r_pot,
):
    ka = lax.axis_index("ka")
    orb = lax.axis_index("orb")
    barrier = pltpu.get_barrier_semaphore()
    for step in (1, 2, 3):
        pl.semaphore_signal(barrier, inc=1, device_id=(ka, (orb + step) % 4), device_id_type=MESH)
    loads = [
        pltpu.make_async_copy(source, target, s_in.at[n])
        for n, (source, target) in enumerate(
            ((fock_hbm, fock), (pot_hbm, pot), (imp_hbm, imp_flat), (pof_hbm, pof))
        )
    ]
    for load in loads:
        load.start()
    for load in loads:
        load.wait()
    m_src[...] = fock[0] + fock[1]
    pl.semaphore_wait(barrier, 3)
    for step in (2, 3, 1):
        to = (orb + step) % 4
        remote(pot, pot_all.at[orb], s_pot.at[step], r_pot.at[step], ka, to).start()
    for step in (2, 3, 1):
        to = (orb + step) % 4
        remote(m_src.at[to], m_all.at[orb], s_fock.at[step], r_fock.at[step], ka, to).start()
    pot_all[orb] = pot[...]
    m_all[orb] = m_src[orb]

    for step in (1, 2, 3):
        remote(pot, pot_all.at[(orb + 4 - step) % 4], s_pot.at[step], r_pot.at[step], ka, orb).wait_recv()
    slot_of = iota((N, 192), 0)
    col_of = iota((N, 192), 1)
    frag_of = slot_of // 48
    pot_of = jnp.zeros((N, 192), jnp.int32)
    for f in range(8):
        pot_of = jnp.where(frag_of == f, pof[f], pot_of)
    pick = ((col_of % 4 == pot_of) & (col_of // 4 == slot_of - 48 * frag_of)).astype(F32)
    stacked = contract(pick, pot_all[...].reshape(192, 48), ((1,), (0,)))
    spread = (iota((48, N), 1) % 48 == iota((48, N), 0)).astype(F32)
    wide = contract(stacked, spread, ((1,), (0,)))
    rows, cols = iota((N, N), 0), iota((N, N), 1)
    wide = jnp.where(rows // 48 == cols // 48, wide, 0.0)
    wide = 0.5 * (wide + wide.T)
    place = (rows == imp_flat[...].reshape(1, N)).astype(F32)
    u_ref[...] = contract(contract(place, wide, ((1,), (0,))), place, ((1,), (1,)))

    for step in (1, 2, 3):
        remote(
            m_src.at[0], m_all.at[(orb + 4 - step) % 4], s_fock.at[step], r_fock.at[step], ka, orb
        ).wait_recv()
    m = m_all[...].reshape(N, N)
    mt = m.T
    scale = 1.0 / bound[0]
    eye = (rows == cols).astype(F32)
    x_out[:, :N] = (0.5 * (m + mt) + u_ref[...] - chem[0] * eye) * scale
    x_out[:, N:] = (0.5 * (m - mt)) * scale
    for step in (1, 2, 3):
        remote(pot, pot_all.at[0], s_pot.at[step], r_pot.at[step], ka, orb).wait_send()
        remote(m_src.at[0], m_all.at[0], s_fock.at[step], r_fock.at[step], ka, orb).wait_send()


def main_kernel(
    x_in, imp_hbm, t_hi, t_lo, landing, f_in,
    imp_flat,
    x_ref, w_hi, w_lo, d_tiles, k_buf, o_buf, d0_buf, full, f_out,
    s_imp, entered, s_k, r_k, s_o, r_o, s_d0, r_d0, s_f, r_f,
):
    ka = lax.axis_index("ka")
    orb = lax.axis_index("orb")
    z, x, yl = ka // 8, (ka // 2) % 4, ka % 2
    yh, core = orb // 2, orb % 2
    me = ka * 4 + orb
    barrier = pltpu.get_barrier_semaphore()

    def greet(d, carry):
        plane = (ka + d // 4) % 8
        pl.semaphore_signal(barrier, inc=1, device_id=(8 * z + plane, (orb + d) % 4), device_id_type=MESH)
        return carry

    fetch = pltpu.make_async_copy(imp_hbm, imp_flat, s_imp)
    fetch.start()
    lax.fori_loop(1, 32, greet, 0)
    for step in range(1, 8):
        pl.semaphore_signal(barrier, inc=1, device_id=((ka + 8 * step) % 64, orb), device_id_type=MESH)

    x_ref[...] = x_in[...]
    rows, cols = iota((N, N), 0), iota((N, N), 1)
    eye = (rows == cols).astype(F32)
    for step in range(ITERS):
        hi, lo = split2(x_ref[...])
        for part, w in ((hi, w_hi), (lo, w_lo)):
            w[:N, :N] = part[:, :N]
            w[:N, N:] = part[:, N:]
            w[N:, :N] = -part[:, N:]
            w[N:, N:] = part[:, :N]
        s = dot3(hi, lo, w_hi[...], w_lo[...])
        s_hi, s_lo = split2(s)
        c = dot3(s_hi, s_lo, w_hi[...], w_lo[...])
        x_ref[...] = 1.5 * x_ref[...] - 0.5 * c
        if step == 0:
            fetch.wait()
            pl.semaphore_wait(barrier, 38)
            for hop in range(1, 8):
                pl.semaphore_signal(entered, inc=1, device_id=((ka + 8 * hop) % 64, orb), device_id_type=MESH)
    values = (0.5 * eye - 0.5 * x_ref[:, :N], -0.5 * x_ref[:, N:])
    for n, (o, p) in enumerate(PAIRS):
        re, im = (pack(v[96 * o : 96 * o + 96, 96 * p : 96 * p + 96]).reshape(9, 8, 128) for v in values)
        for half in range(2):
            rows_at = slice(4 * half, 4 * half + 4)
            d_tiles[18 * n + 9 * half : 18 * n + 9 * half + 9] = jnp.concatenate(
                [re[:, rows_at], im[:, rows_at]], axis=1
            )

    column = column_of(x, yl, yh)
    first, second, has_second = tiles_at(z, column)
    own_tile = jnp.where(core == 1, first, second)
    has_tile = (core == 1) | has_second
    pl.semaphore_wait(entered, 7)

    def spread_k(d, carry):
        to_z = (z + far_then_near(d % 8)) % 8
        to_x = (x + (d // 8) % 4) % 4
        to_yl = (yl + (d // 32) % 2) % 2
        to_yh = (yh + d // 64) % 2
        to_first, to_second, there = tiles_at(to_z, column_of(to_x, to_yl, to_yh))
        to_ka = to_z * 8 + to_x * 2 + to_yl

        @pl.when((d != 7) | (core == 0))
        def _():
            remote(d_tiles.at[to_first], k_buf.at[me], s_k, r_k, to_ka, to_yh * 2 + 1).start()

        @pl.when(there & ((d != 7) | (core == 1)))
        def _():
            remote(d_tiles.at[to_second], k_buf.at[me], s_k, r_k, to_ka, to_yh * 2).start()

        return carry

    lax.fori_loop(0, 128, spread_k, 0)
    t_o, t_p = blocks_of(own_tile // 18)
    t_m = own_tile % 18
    mirrored = t_o != t_p
    to_self = (t_o == orb) | (t_p == orb)

    @pl.when(has_tile)
    def _():
        k_buf[me] = d_tiles[own_tile]
        wait_bytes(k_buf.at[pl.ds(0, K - 1)], r_k)
        k_rows = k_buf.reshape(K * 8, 128)
        o_rows = o_buf.reshape(2 * K * 8, 128)
        for s in range(4):
            both = [k_rows[pl.ds(c * 4 + s, K, stride=8), :] for c in range(2)]
            v_hi, v_lo = split2(jnp.concatenate(both, axis=1))
            res = dot3(t_hi[...], t_lo[...], v_hi, v_lo)
            cos_re, cos_im = res[:K, :128], res[:K, 128:]
            sin_re, sin_im = res[K:, :128], res[K:, 128:]
            o_rows[pl.ds(s, K, stride=8), :] = cos_re - sin_im
            o_rows[pl.ds(4 + s, K, stride=8), :] = cos_im + sin_re
            o_rows[pl.ds(K * 8 + s, K, stride=8), :] = cos_re + sin_im
            o_rows[pl.ds(K * 8 + 4 + s, K, stride=8), :] = sin_re - cos_im

        def send_d0(g, carry):
            to_ka, to_orb = frag_device(g)
            remote(o_buf.at[0, 0], d0_buf.at[own_tile], s_d0, r_d0, to_ka, to_orb).start()
            return carry

        lax.fori_loop(0, 8, send_d0, 0)

        def send_o(d, carry):
            to_z = (z + far_then_near(d % 8)) % 8
            to_x = (x + (d // 8) % 4) % 4
            to_yl = (yl + d // 32) % 2
            to_ka = to_z * 8 + to_x * 2 + to_yl
            cells_at = pl.ds(4 * to_ka, 4)

            @pl.when((d != 7) | (t_o != orb))
            def _():
                remote(o_buf.at[0, cells_at], landing.at[t_p * 18 + t_m], s_o, r_o, to_ka, t_o).start()

            @pl.when(mirrored & ((d != 7) | (t_p != orb)))
            def _():
                remote(o_buf.at[1, cells_at], landing.at[t_o * 18 + t_m], s_o, r_o, to_ka, t_p).start()

            return carry

        lax.fori_loop(0, 64, send_o, 0)

        @pl.when(t_o == orb)
        def _():
            landing[t_p * 18 + t_m] = o_buf[0, pl.ds(4 * ka, 4)]

        @pl.when(mirrored & (t_p == orb))
        def _():
            landing[t_o * 18 + t_m] = o_buf[1, pl.ds(4 * ka, 4)]

    f_o, f_half = z % 4, z // 4
    makes = (core == 0) & (column == (z + 6) % 8)

    @pl.when(makes)
    def _():
        imp = imp_flat[...].reshape(1, N)
        slots = [imp[:, 96 * o : 96 * o + 96] for o in range(4)]
        own_slots = slots[0]
        for o in range(1, 4):
            own_slots = jnp.where(f_o == o, slots[o], own_slots)
        own_slots = jnp.concatenate([own_slots, jnp.full((1, 32), -1, jnp.int32)], axis=1)
        wait_bytes(d0_buf, r_d0)
        chosen = (iota((N, 128), 0) == own_slots).astype(F32)
        left = iota((48, 128), 1) < 48
        for part in range(2):
            for n, (o, p) in enumerate(PAIRS):
                halves = [d0_buf[18 * n + 9 * h : 18 * n + 9 * h + 9, 4 * part : 4 * part + 4] for h in range(2)]
                block = unpack(jnp.concatenate(halves, axis=1).reshape(72, 128))
                full[96 * o : 96 * o + 96, 96 * p : 96 * p + 96] = block
                if o != p:
                    full[96 * p : 96 * p + 96, 96 * o : 96 * o + 96] = block.T if part == 0 else -block.T
            picked = contract(contract(chosen, full[...], ((0,), (0,))), chosen, ((1,), (0,)))
            f_out[part] = jnp.where(left, picked[:48], picked[48:96])

        def send_f(d, carry):
            to_ka = ((z + far_then_near(d % 8)) % 8) * 8 + (ka + d // 8) % 8
            rows_at = pl.ds(pl.multiple_of(24 * f_half, 8), 24)
            remote(f_out.at[:, rows_at], f_in.at[:, rows_at], s_f, r_f, to_ka, f_o).start()
            return carry

        lax.fori_loop(0, 64, send_f, 0)

    wait_bytes(f_in, r_f)
    keeps = has_tile & to_self

    @pl.when(keeps)
    def _():
        wait_bytes(landing.at[pl.ds(0, 71)], r_o)

    @pl.when(jnp.logical_not(keeps))
    def _():
        wait_bytes(landing, r_o)

    @pl.when(has_tile)
    def _():
        wait_bytes(d_tiles.at[pl.ds(0, TILES - 1)], s_k)
        wait_bytes(d_tiles.at[pl.ds(0, 8)], s_d0)

    @pl.when(jnp.logical_not(has_tile))
    def _():
        wait_bytes(d_tiles, s_k)

    for side, sent, fewer in (
        (mirrored, o_buf, o_buf.at[:, pl.ds(0, K - 2)]),
        (jnp.logical_not(mirrored), o_buf.at[0], o_buf.at[0, pl.ds(0, K - 4)]),
    ):

        @pl.when(has_tile & side & to_self)
        def _(fewer=fewer):
            wait_bytes(fewer, s_o)

        @pl.when(has_tile & side & jnp.logical_not(to_self))
        def _(sent=sent):
            wait_bytes(sent, s_o)

    @pl.when(makes)
    def _():
        wait_bytes(o_buf.at[:, pl.ds(0, 192)], s_f)


def store_kernel(landing, f_in, out, frag, buf, sem):
    own = lax.axis_index("orb")
    stores = [
        [pltpu.make_async_copy(buf.at[c, r], out.at[c, r], sem.at[c, r]) for r in range(4)] for c in range(2)
    ]
    for place in range(4):

        @pl.when(own == place)
        def _(place=place):
            for r in range(4):
                for c in range(2):
                    blocks = []
                    for q in range(4):
                        halves = [
                            landing[18 * q + 9 * h : 18 * q + 9 * h + 9, r, 4 * c : 4 * c + 4] for h in range(2)
                        ]
                        block = unpack(jnp.concatenate(halves, axis=1).reshape(72, 128))
                        blocks.append(block if place <= q else block.T)
                    buf[c, r] = jnp.concatenate(blocks, axis=1)
                    stores[c][r].start()

    for part in range(2):
        for f in range(2):
            frag[part, f] = f_in[part, :, 48 * f : 48 * f + 48]
    for store in stores[0] + stores[1]:
        store.wait()


def tables():
    grid = np.outer(np.arange(K), np.arange(K)) % K
    angle = grid * (2.0 * math.pi / K)
    c, s = np.cos(angle) / K, np.sin(angle) / K
    full = np.concatenate([c, s]).astype(np.float32)
    hi = full.astype(jnp.bfloat16)
    lo = (full - hi.astype(np.float32)).astype(jnp.bfloat16)
    return hi, lo


def per_device(fock, potential, chem_potential, spectral_bound, impurity_orbitals, potential_of):
    t_hi, t_lo = tables()
    vmem = pl.BlockSpec(memory_space=pltpu.VMEM)
    smem = pl.BlockSpec(memory_space=pltpu.SMEM)
    hbm = pl.BlockSpec(memory_space=pltpu.HBM)
    dma = pltpu.SemaphoreType.DMA
    pot = potential.transpose(1, 0, 2).reshape(48, 48)
    imp = pltpu.with_memory_space_constraint(impurity_orbitals, pltpu.HBM)
    start = pl.pallas_call(
        gather_kernel,
        name="gather",
        out_shape=jax.ShapeDtypeStruct((N, 2 * N), F32),
        in_specs=[hbm, hbm, smem, smem, hbm, hbm],
        out_specs=vmem,
        scratch_shapes=[
            pltpu.VMEM((2, 4, 96, N), F32),
            pltpu.VMEM((48, 48), F32),
            pltpu.VMEM((N,), jnp.int32),
            pltpu.SMEM((8,), jnp.int32),
            pltpu.VMEM((4, 96, N), F32),
            pltpu.VMEM((4, 96, N), F32),
            pltpu.VMEM((4, 48, 48), F32),
            pltpu.VMEM((N, N), F32),
            dma((4,)), dma((4,)), dma((4,)), dma((4,)), dma((4,)),
        ],
        compiler_params=pltpu.CompilerParams(
            has_side_effects=True, collective_id=0, vmem_limit_bytes=40 << 20
        ),
    )(
        pltpu.with_memory_space_constraint(fock, pltpu.HBM),
        pltpu.with_memory_space_constraint(pot, pltpu.HBM),
        chem_potential,
        spectral_bound,
        imp,
        pltpu.with_memory_space_constraint(potential_of, pltpu.HBM),
    )
    landing, f_in = pl.pallas_call(
        main_kernel,
        name="transform",
        out_shape=(
            jax.ShapeDtypeStruct((72, 4, 8, 128), F32),
            jax.ShapeDtypeStruct((2, 48, 128), F32),
        ),
        in_specs=[vmem, hbm, vmem, vmem],
        out_specs=(vmem, vmem),
        scratch_shapes=[
            pltpu.VMEM((N,), jnp.int32),
            pltpu.VMEM((N, 2 * N), F32),
            pltpu.VMEM((2 * N, 2 * N), BF16),
            pltpu.VMEM((2 * N, 2 * N), BF16),
            pltpu.VMEM((TILES, 8, 128), F32),
            pltpu.VMEM((K, 8, 128), F32),
            pltpu.VMEM((2, K, 8, 128), F32),
            pltpu.VMEM((TILES, 8, 128), F32),
            pltpu.VMEM((N, N), F32),
            pltpu.VMEM((2, 48, 128), F32),
            dma,
            pltpu.SemaphoreType.REGULAR,
            dma, dma, dma, dma, dma, dma, dma, dma,
        ],
        compiler_params=pltpu.CompilerParams(
            has_side_effects=True, collective_id=1, vmem_limit_bytes=48 << 20
        ),
    )(start, imp, jnp.asarray(t_hi), jnp.asarray(t_lo))
    return pl.pallas_call(
        store_kernel,
        name="store",
        out_shape=(
            jax.ShapeDtypeStruct((2, 4, 96, N), F32),
            jax.ShapeDtypeStruct((2, 2, 48, 48), F32),
        ),
        in_specs=[vmem, vmem],
        out_specs=(hbm, vmem),
        scratch_shapes=[pltpu.VMEM((2, 4, 96, N), F32), dma((2, 4))],
        compiler_params=pltpu.CompilerParams(vmem_limit_bytes=8 << 20),
    )(landing, f_in)


def solution(mesh):
    return jax.shard_map(
        per_device,
        mesh=mesh,
        in_specs=(P(None, "ka", "orb", None), P(None, "orb", None), P(), P(), P(), P()),
        out_specs=(P(None, "ka", "orb", None), P(None, "orb", None, None)),
        check_vma=False,
    )
```

```python
import functools
import math

import jax
import jax.numpy as jnp
import numpy as np
from jax import lax
from jax.experimental import pallas as pl
from jax.experimental.pallas import tpu as pltpu
from jax.sharding import PartitionSpec as P

ITERS = 2
N = 384
K = 256
F32 = jnp.float32
BF16 = jnp.bfloat16
MESH = pl.DeviceIdType.MESH


def split2(x):
    hi = x.astype(BF16)
    return hi, (x - hi.astype(F32)).astype(BF16)


def dot(a, b):
    return jnp.dot(a, b, preferred_element_type=F32)


def dot3(a_hi, a_lo, b_hi, b_lo):
    return dot(a_hi, b_hi) + (dot(a_hi, b_lo) + dot(a_lo, b_hi))


def contract(a, b, dims):
    return lax.dot_general(
        a, b, (dims, ((), ())), precision=lax.Precision.HIGHEST, preferred_element_type=F32
    )


def iota(shape, dim):
    return lax.broadcasted_iota(jnp.int32, shape, dim)


def remote(src, dst, send, recv, ka, orb):
    return pltpu.make_async_remote_copy(
        src_ref=src, dst_ref=dst, send_sem=send, recv_sem=recv, device_id=(ka, orb), device_id_type=MESH
    )


def wait_bytes(ref, sem):
    pltpu.make_async_copy(ref, ref, sem).wait()


PAIRS = ((0, 1), (0, 2), (0, 3), (1, 2), (1, 3), (2, 3), (0, 0), (1, 1), (2, 2), (3, 3))
TILES = 18 * len(PAIRS)


def pack(block):
    a, b, c, d = (block[24 * n : 24 * n + 24] for n in range(4))
    return jnp.concatenate(
        [
            jnp.concatenate([a, b[:, :32]], axis=1),
            jnp.concatenate([b[:, 32:], c[:, :64]], axis=1),
            jnp.concatenate([c[:, 64:], d], axis=1),
        ],
        axis=0,
    )


def unpack(packed):
    p, q, r = (packed[24 * n : 24 * n + 24] for n in range(3))
    return jnp.concatenate(
        [
            p[:, :96],
            jnp.concatenate([p[:, 96:], q[:, :64]], axis=1),
            jnp.concatenate([q[:, 64:], r[:, :32]], axis=1),
            r[:, 32:],
        ],
        axis=0,
    )


def blocks_of(pair):
    late, last = (pair >= 3).astype(jnp.int32), (pair >= 5).astype(jnp.int32)
    diagonal = pair >= 6
    return (
        jnp.where(diagonal, pair - 6, late + last),
        jnp.where(diagonal, pair - 6, pair + 1 - 2 * late - last),
    )


def slots():
    at = {}
    for column in range(16):
        for turn in range(8):
            tile = turn * 16 + column
            if turn == 7:
                tile = 124 + column
            elif turn == 6 and column >= 12:
                tile = 164 + column
            at[tile] = turn * 16 + column
        for n, first in enumerate((108, 140, 156)):
            at[first + column] = 128 + 16 * n + column
        if column >= 12:
            at[160 + column] = 164 + column
    return at


def own_tiles(turn, column):
    late = (turn == 6) & (column >= 12)
    first = jnp.where(turn == 7, 124 + column, jnp.where(late, 164 + column, turn * 16 + column))
    second = jnp.where(turn == 7, 108, jnp.where(turn == 1, 140, jnp.where(turn == 5, 156, 160))) + column
    slot = jnp.where(turn == 7, 128, jnp.where(turn == 1, 144, jnp.where(turn == 5, 160, 164))) + column
    return first, turn * 16 + column, second, slot, (turn == 7) | (turn == 1) | (turn == 5) | late


STEPS = (4, 3, 5, 2, 6, 1, 7, 0)


def frag_device(g):
    column = (g + 6) % 8
    return 8 * g + 2 * (column // 4) + column % 2, 2 * ((column // 2) % 2)


def gather_kernel(
    fock_hbm, pot_hbm, chem, bound, imp_hbm, pof_hbm, x_out,
    fock, pot, imp_flat, pof, m_src, m_all, pot_all, u_ref, s_in, s_fock, r_fock, s_pot, r_pot,
):
    ka = lax.axis_index("ka")
    orb = lax.axis_index("orb")
    barrier = pltpu.get_barrier_semaphore()
    for step in (1, 2, 3):
        pl.semaphore_signal(barrier, inc=1, device_id=(ka, (orb + step) % 4), device_id_type=MESH)
    loads = [
        pltpu.make_async_copy(source, target, s_in.at[n])
        for n, (source, target) in enumerate(
            ((fock_hbm, fock), (pot_hbm, pot), (imp_hbm, imp_flat), (pof_hbm, pof))
        )
    ]
    for load in loads:
        load.start()
    for load in loads:
        load.wait()
    m_src[...] = fock[0] + fock[1]
    pl.semaphore_wait(barrier, 3)
    for step in (2, 3, 1):
        to = (orb + step) % 4
        remote(pot, pot_all.at[orb], s_pot.at[step], r_pot.at[step], ka, to).start()
    for step in (2, 3, 1):
        to = (orb + step) % 4
        remote(m_src.at[to], m_all.at[orb], s_fock.at[step], r_fock.at[step], ka, to).start()
    pot_all[orb] = pot[...]
    m_all[orb] = m_src[orb]

    for step in (1, 2, 3):
        remote(pot, pot_all.at[(orb + 4 - step) % 4], s_pot.at[step], r_pot.at[step], ka, orb).wait_recv()
    slot_of = iota((N, 192), 0)
    col_of = iota((N, 192), 1)
    frag_of = slot_of // 48
    pot_of = jnp.zeros((N, 192), jnp.int32)
    for f in range(8):
        pot_of = jnp.where(frag_of == f, pof[f], pot_of)
    pick = ((col_of % 4 == pot_of) & (col_of // 4 == slot_of - 48 * frag_of)).astype(F32)
    stacked = contract(pick, pot_all[...].reshape(192, 48), ((1,), (0,)))
    spread = (iota((48, N), 1) % 48 == iota((48, N), 0)).astype(F32)
    wide = contract(stacked, spread, ((1,), (0,)))
    rows, cols = iota((N, N), 0), iota((N, N), 1)
    wide = jnp.where(rows // 48 == cols // 48, wide, 0.0)
    wide = 0.5 * (wide + wide.T)
    place = (rows == imp_flat[...].reshape(1, N)).astype(F32)
    u_ref[...] = contract(contract(place, wide, ((1,), (0,))), place, ((1,), (1,)))

    for step in (1, 2, 3):
        remote(
            m_src.at[0], m_all.at[(orb + 4 - step) % 4], s_fock.at[step], r_fock.at[step], ka, orb
        ).wait_recv()
    m = m_all[...].reshape(N, N)
    mt = m.T
    scale = 1.0 / bound[0]
    eye = (rows == cols).astype(F32)
    x_out[:, :N] = (0.5 * (m + mt) + u_ref[...] - chem[0] * eye) * scale
    x_out[:, N:] = (0.5 * (m - mt)) * scale
    for step in (1, 2, 3):
        remote(pot, pot_all.at[0], s_pot.at[step], r_pot.at[step], ka, orb).wait_send()
        remote(m_src.at[0], m_all.at[0], s_fock.at[step], r_fock.at[step], ka, orb).wait_send()


def main_kernel(
    x_in, imp_hbm, t_hi, t_lo, landing, f_in,
    imp_flat,
    x_ref, w_hi, w_lo, d_tiles, k_buf, o_buf, d0_buf, full, f_out,
    s_imp, entered, s_k, r_k, s_o, r_o, s_d0, r_d0, s_f, r_f,
):
    ka = lax.axis_index("ka")
    orb = lax.axis_index("orb")
    z, x, yl = ka // 8, (ka // 2) % 4, ka % 2
    yh, core = orb // 2, orb % 2
    me = ka * 4 + orb
    barrier = pltpu.get_barrier_semaphore()

    def greet(d, carry):
        plane = (ka + d // 4) % 8
        pl.semaphore_signal(barrier, inc=1, device_id=(8 * z + plane, (orb + d) % 4), device_id_type=MESH)
        return carry

    fetch = pltpu.make_async_copy(imp_hbm, imp_flat, s_imp)
    fetch.start()
    lax.fori_loop(1, 32, greet, 0)
    for step in range(1, 8):
        pl.semaphore_signal(barrier, inc=1, device_id=((ka + 8 * step) % 64, orb), device_id_type=MESH)

    x_ref[...] = x_in[...]
    rows, cols = iota((N, N), 0), iota((N, N), 1)
    eye = (rows == cols).astype(F32)
    for step in range(ITERS):
        hi, lo = split2(x_ref[...])
        for part, w in ((hi, w_hi), (lo, w_lo)):
            w[:N, :N] = part[:, :N]
            w[:N, N:] = part[:, N:]
            w[N:, :N] = -part[:, N:]
            w[N:, N:] = part[:, :N]
        s = dot3(hi, lo, w_hi[...], w_lo[...])
        s_hi, s_lo = split2(s)
        c = dot3(s_hi, s_lo, w_hi[...], w_lo[...])
        x_ref[...] = 1.5 * x_ref[...] - 0.5 * c
        if step == 0:
            fetch.wait()
            pl.semaphore_wait(barrier, 38)
            for hop in range(1, 8):
                pl.semaphore_signal(entered, inc=1, device_id=((ka + 8 * hop) % 64, orb), device_id_type=MESH)
    slot_of_tile = slots()
    values = (0.5 * eye - 0.5 * x_ref[:, :N], -0.5 * x_ref[:, N:])
    for n, (o, p) in enumerate(PAIRS):
        re, im = (pack(v[96 * o : 96 * o + 96, 96 * p : 96 * p + 96]).reshape(9, 8, 128) for v in values)
        for half in range(2):
            rows_at = slice(4 * half, 4 * half + 4)
            quads = jnp.concatenate([re[:, rows_at], im[:, rows_at]], axis=1)
            for t in range(9):
                d_tiles[slot_of_tile[18 * n + 9 * half + t]] = quads[t]

    column = x * 4 + yh * 2 + yl
    turn = lax.rem(z + 16 - column, 8)
    first, first_slot, second, second_slot, has_second = own_tiles(turn, column)
    own_tile = jnp.where(core == 1, first, second)
    own_slot = jnp.where(core == 1, first_slot, second_slot)
    has_tile = (core == 1) | has_second
    pl.semaphore_wait(entered, 7)

    def send_k(slot, to_ka, to_orb):
        remote(d_tiles.at[slot], k_buf.at[me], s_k, r_k, to_ka, to_orb).start()

    def column_at(e):
        to_x = lax.rem(x + lax.rem(e, 4), 4)
        to_yl = lax.rem(yl + lax.rem(lax.div(e, 4), 2), 2)
        to_yh = lax.rem(yh + lax.div(e, 8), 2)
        return to_x * 4 + to_yh * 2 + to_yl, to_x * 2 + to_yl, to_yh * 2

    def spread_first(e, carry):
        to_column, to_line, to_orb = column_at(e)
        for step in STEPS:
            to_z = lax.rem(z + step, 8)
            slot = lax.rem(to_z + 16 - to_column, 8) * 16 + to_column
            if step:
                send_k(slot, to_z * 8 + to_line, to_orb + 1)
            else:

                @pl.when((e > 0) | (core == 0))
                def _(slot=slot, to_z=to_z):
                    send_k(slot, to_z * 8 + to_line, to_orb + 1)

        return carry

    lax.fori_loop(0, 16, spread_first, 0)

    def spread_second(e, carry):
        to_column, to_line, to_orb = column_at(e)
        for n, to_turn in enumerate((7, 1, 5)):
            to_z = lax.rem(to_turn + to_column, 8)

            @pl.when((e > 0) | (core == 1) | (to_z != z))
            def _(n=n, to_z=to_z):
                send_k(128 + 16 * n + to_column, to_z * 8 + to_line, to_orb)

        return carry

    lax.fori_loop(0, 16, spread_second, 0)

    def spread_late(e, carry):
        place = lax.rem(e + column, 4)
        to_column = 12 + place
        to_z = lax.rem(6 + to_column, 8)

        @pl.when((to_column != column) | (core == 1) | (to_z != z))
        def _():
            send_k(164 + to_column, to_z * 8 + 6 + lax.rem(place, 2), 2 * lax.div(place, 2))

        return carry

    lax.fori_loop(0, 4, spread_late, 0)
    t_o, t_p = blocks_of(own_tile // 18)
    t_m = own_tile % 18
    mirrored = t_o != t_p
    to_self = (t_o == orb) | (t_p == orb)

    @pl.when(has_tile)
    def _():
        k_buf[me] = d_tiles[own_slot]
        wait_bytes(k_buf.at[pl.ds(0, K - 1)], r_k)
        k_rows = k_buf.reshape(K * 8, 128)
        o_rows = o_buf.reshape(2 * K * 8, 128)
        for s in range(4):
            both = [k_rows[pl.ds(c * 4 + s, K, stride=8), :] for c in range(2)]
            v_hi, v_lo = split2(jnp.concatenate(both, axis=1))
            res = dot3(t_hi[...], t_lo[...], v_hi, v_lo)
            cos_re, cos_im = res[:K, :128], res[:K, 128:]
            sin_re, sin_im = res[K:, :128], res[K:, 128:]
            o_rows[pl.ds(s, K, stride=8), :] = cos_re - sin_im
            o_rows[pl.ds(4 + s, K, stride=8), :] = cos_im + sin_re
            o_rows[pl.ds(K * 8 + s, K, stride=8), :] = cos_re + sin_im
            o_rows[pl.ds(K * 8 + 4 + s, K, stride=8), :] = sin_re - cos_im

        def send_d0(g, carry):
            to_ka, to_orb = frag_device(g)
            remote(o_buf.at[0, 0], d0_buf.at[own_tile], s_d0, r_d0, to_ka, to_orb).start()
            return carry

        lax.fori_loop(0, 8, send_d0, 0)

        def send_o(e, carry):
            to_x = lax.rem(x + lax.rem(e, 4), 4)
            to_yl = lax.rem(yl + lax.div(e, 4), 2)
            to_line = to_x * 2 + to_yl

            def send_side(side, place, to_orb):
                for step in STEPS:
                    to_ka = lax.rem(z + step, 8) * 8 + to_line

                    def send(to_ka=to_ka):
                        cells_at = o_buf.at[side, pl.ds(4 * to_ka, 4)]
                        remote(cells_at, landing.at[place], s_o, r_o, to_ka, to_orb).start()

                    if step:
                        send()
                    else:
                        pl.when((e > 0) | (to_orb != orb))(send)

            send_side(0, t_p * 18 + t_m, t_o)

            @pl.when(mirrored)
            def _():
                send_side(1, t_o * 18 + t_m, t_p)

            return carry

        lax.fori_loop(0, 8, send_o, 0)

        @pl.when(t_o == orb)
        def _():
            landing[t_p * 18 + t_m] = o_buf[0, pl.ds(4 * ka, 4)]

        @pl.when(mirrored & (t_p == orb))
        def _():
            landing[t_o * 18 + t_m] = o_buf[1, pl.ds(4 * ka, 4)]

    f_o, f_half = z % 4, z // 4
    makes = (core == 0) & (column == (z + 6) % 8)

    @pl.when(makes)
    def _():
        imp = imp_flat[...].reshape(1, N)
        slots = [imp[:, 96 * o : 96 * o + 96] for o in range(4)]
        own_slots = slots[0]
        for o in range(1, 4):
            own_slots = jnp.where(f_o == o, slots[o], own_slots)
        own_slots = jnp.concatenate([own_slots, jnp.full((1, 32), -1, jnp.int32)], axis=1)
        wait_bytes(d0_buf, r_d0)
        chosen = (iota((N, 128), 0) == own_slots).astype(F32)
        left = iota((48, 128), 1) < 48
        for part in range(2):
            for n, (o, p) in enumerate(PAIRS):
                halves = [d0_buf[18 * n + 9 * h : 18 * n + 9 * h + 9, 4 * part : 4 * part + 4] for h in range(2)]
                block = unpack(jnp.concatenate(halves, axis=1).reshape(72, 128))
                full[96 * o : 96 * o + 96, 96 * p : 96 * p + 96] = block
                if o != p:
                    full[96 * p : 96 * p + 96, 96 * o : 96 * o + 96] = block.T if part == 0 else -block.T
            picked = contract(contract(chosen, full[...], ((0,), (0,))), chosen, ((1,), (0,)))
            f_out[part] = jnp.where(left, picked[:48], picked[48:96])

        def send_f(d, carry):
            to_ka = lax.rem(z + lax.rem(d * 3 + 4, 8), 8) * 8 + lax.rem(ka + lax.div(d, 8), 8)
            rows_at = pl.ds(pl.multiple_of(24 * f_half, 8), 24)
            remote(f_out.at[:, rows_at], f_in.at[:, rows_at], s_f, r_f, to_ka, f_o).start()
            return carry

        lax.fori_loop(0, 64, send_f, 0)

    wait_bytes(f_in, r_f)
    keeps = has_tile & to_self

    @pl.when(keeps)
    def _():
        wait_bytes(landing.at[pl.ds(0, 71)], r_o)

    @pl.when(jnp.logical_not(keeps))
    def _():
        wait_bytes(landing, r_o)

    @pl.when(has_tile)
    def _():
        wait_bytes(d_tiles.at[pl.ds(0, TILES - 1)], s_k)
        wait_bytes(d_tiles.at[pl.ds(0, 8)], s_d0)

    @pl.when(jnp.logical_not(has_tile))
    def _():
        wait_bytes(d_tiles, s_k)

    for side, sent, fewer in (
        (mirrored, o_buf, o_buf.at[:, pl.ds(0, K - 2)]),
        (jnp.logical_not(mirrored), o_buf.at[0], o_buf.at[0, pl.ds(0, K - 4)]),
    ):

        @pl.when(has_tile & side & to_self)
        def _(fewer=fewer):
            wait_bytes(fewer, s_o)

        @pl.when(has_tile & side & jnp.logical_not(to_self))
        def _(sent=sent):
            wait_bytes(sent, s_o)

    @pl.when(makes)
    def _():
        wait_bytes(o_buf.at[:, pl.ds(0, 192)], s_f)


def store_kernel(landing, f_in, out, frag, buf, sem):
    own = lax.axis_index("orb")
    stores = [
        [pltpu.make_async_copy(buf.at[c, r], out.at[c, r], sem.at[c, r]) for r in range(4)] for c in range(2)
    ]
    for place in range(4):

        @pl.when(own == place)
        def _(place=place):
            for r in range(4):
                for c in range(2):
                    blocks = []
                    for q in range(4):
                        halves = [
                            landing[18 * q + 9 * h : 18 * q + 9 * h + 9, r, 4 * c : 4 * c + 4] for h in range(2)
                        ]
                        block = unpack(jnp.concatenate(halves, axis=1).reshape(72, 128))
                        blocks.append(block if place <= q else block.T)
                    buf[c, r] = jnp.concatenate(blocks, axis=1)
                    stores[c][r].start()

    for part in range(2):
        for f in range(2):
            frag[part, f] = f_in[part, :, 48 * f : 48 * f + 48]
    for store in stores[0] + stores[1]:
        store.wait()


def tables():
    grid = np.outer(np.arange(K), np.arange(K)) % K
    angle = grid * (2.0 * math.pi / K)
    c, s = np.cos(angle) / K, np.sin(angle) / K
    full = np.concatenate([c, s]).astype(np.float32)
    hi = full.astype(jnp.bfloat16)
    lo = (full - hi.astype(np.float32)).astype(jnp.bfloat16)
    return hi, lo


def per_device(fock, potential, chem_potential, spectral_bound, impurity_orbitals, potential_of):
    t_hi, t_lo = tables()
    vmem = pl.BlockSpec(memory_space=pltpu.VMEM)
    smem = pl.BlockSpec(memory_space=pltpu.SMEM)
    hbm = pl.BlockSpec(memory_space=pltpu.HBM)
    dma = pltpu.SemaphoreType.DMA
    pot = potential.transpose(1, 0, 2).reshape(48, 48)
    imp = pltpu.with_memory_space_constraint(impurity_orbitals, pltpu.HBM)
    start = pl.pallas_call(
        gather_kernel,
        name="gather",
        out_shape=jax.ShapeDtypeStruct((N, 2 * N), F32),
        in_specs=[hbm, hbm, smem, smem, hbm, hbm],
        out_specs=vmem,
        scratch_shapes=[
            pltpu.VMEM((2, 4, 96, N), F32),
            pltpu.VMEM((48, 48), F32),
            pltpu.VMEM((N,), jnp.int32),
            pltpu.SMEM((8,), jnp.int32),
            pltpu.VMEM((4, 96, N), F32),
            pltpu.VMEM((4, 96, N), F32),
            pltpu.VMEM((4, 48, 48), F32),
            pltpu.VMEM((N, N), F32),
            dma((4,)), dma((4,)), dma((4,)), dma((4,)), dma((4,)),
        ],
        compiler_params=pltpu.CompilerParams(
            has_side_effects=True, collective_id=0, vmem_limit_bytes=40 << 20
        ),
    )(
        pltpu.with_memory_space_constraint(fock, pltpu.HBM),
        pltpu.with_memory_space_constraint(pot, pltpu.HBM),
        chem_potential,
        spectral_bound,
        imp,
        pltpu.with_memory_space_constraint(potential_of, pltpu.HBM),
    )
    landing, f_in = pl.pallas_call(
        main_kernel,
        name="transform",
        out_shape=(
            jax.ShapeDtypeStruct((72, 4, 8, 128), F32),
            jax.ShapeDtypeStruct((2, 48, 128), F32),
        ),
        in_specs=[vmem, hbm, vmem, vmem],
        out_specs=(vmem, vmem),
        scratch_shapes=[
            pltpu.VMEM((N,), jnp.int32),
            pltpu.VMEM((N, 2 * N), F32),
            pltpu.VMEM((2 * N, 2 * N), BF16),
            pltpu.VMEM((2 * N, 2 * N), BF16),
            pltpu.VMEM((TILES, 8, 128), F32),
            pltpu.VMEM((K, 8, 128), F32),
            pltpu.VMEM((2, K, 8, 128), F32),
            pltpu.VMEM((TILES, 8, 128), F32),
            pltpu.VMEM((N, N), F32),
            pltpu.VMEM((2, 48, 128), F32),
            dma,
            pltpu.SemaphoreType.REGULAR,
            dma, dma, dma, dma, dma, dma, dma, dma,
        ],
        compiler_params=pltpu.CompilerParams(
            has_side_effects=True, collective_id=1, vmem_limit_bytes=48 << 20
        ),
    )(start, imp, jnp.asarray(t_hi), jnp.asarray(t_lo))
    return pl.pallas_call(
        store_kernel,
        name="store",
        out_shape=(
            jax.ShapeDtypeStruct((2, 4, 96, N), F32),
            jax.ShapeDtypeStruct((2, 2, 48, 48), F32),
        ),
        in_specs=[vmem, vmem],
        out_specs=(hbm, vmem),
        scratch_shapes=[pltpu.VMEM((2, 4, 96, N), F32), dma((2, 4))],
        compiler_params=pltpu.CompilerParams(vmem_limit_bytes=8 << 20),
    )(landing, f_in)


def solution(mesh):
    return jax.shard_map(
        per_device,
        mesh=mesh,
        in_specs=(P(None, "ka", "orb", None), P(None, "orb", None), P(), P(), P(), P()),
        out_specs=(P(None, "ka", "orb", None), P(None, "orb", None, None)),
        check_vma=False,
    )
```

```python
import functools
import math

import jax
import jax.numpy as jnp
import numpy as np
from jax import lax
from jax.experimental import pallas as pl
from jax.experimental.pallas import tpu as pltpu
from jax.sharding import PartitionSpec as P

ITERS = 2
N = 384
K = 256
F32 = jnp.float32
BF16 = jnp.bfloat16
MESH = pl.DeviceIdType.MESH


def split2(x):
    hi = x.astype(BF16)
    return hi, (x - hi.astype(F32)).astype(BF16)


def dot(a, b):
    return jnp.dot(a, b, preferred_element_type=F32)


def dot3(a_hi, a_lo, b_hi, b_lo):
    return dot(a_hi, b_hi) + (dot(a_hi, b_lo) + dot(a_lo, b_hi))


def contract(a, b, dims):
    return lax.dot_general(
        a, b, (dims, ((), ())), precision=lax.Precision.HIGHEST, preferred_element_type=F32
    )


def iota(shape, dim):
    return lax.broadcasted_iota(jnp.int32, shape, dim)


def remote(src, dst, send, recv, ka, orb):
    return pltpu.make_async_remote_copy(
        src_ref=src, dst_ref=dst, send_sem=send, recv_sem=recv, device_id=(ka, orb), device_id_type=MESH
    )


def wait_bytes(ref, sem):
    pltpu.make_async_copy(ref, ref, sem).wait()


PAIRS = ((0, 1), (0, 2), (0, 3), (1, 2), (1, 3), (2, 3), (0, 0), (1, 1), (2, 2), (3, 3))
TILES = 18 * len(PAIRS)


def pack(block):
    a, b, c, d = (block[24 * n : 24 * n + 24] for n in range(4))
    return jnp.concatenate(
        [
            jnp.concatenate([a, b[:, :32]], axis=1),
            jnp.concatenate([b[:, 32:], c[:, :64]], axis=1),
            jnp.concatenate([c[:, 64:], d], axis=1),
        ],
        axis=0,
    )


def unpack(packed):
    p, q, r = (packed[24 * n : 24 * n + 24] for n in range(3))
    return jnp.concatenate(
        [
            p[:, :96],
            jnp.concatenate([p[:, 96:], q[:, :64]], axis=1),
            jnp.concatenate([q[:, 64:], r[:, :32]], axis=1),
            r[:, 32:],
        ],
        axis=0,
    )


def blocks_of(pair):
    late, last = (pair >= 3).astype(jnp.int32), (pair >= 5).astype(jnp.int32)
    diagonal = pair >= 6
    return (
        jnp.where(diagonal, pair - 6, late + last),
        jnp.where(diagonal, pair - 6, pair + 1 - 2 * late - last),
    )


def slots():
    at = {}
    for column in range(16):
        for turn in range(8):
            tile = turn * 16 + column
            if turn == 7:
                tile = 124 + column
            elif turn == 6 and column >= 12:
                tile = 164 + column
            at[tile] = turn * 16 + column
        for n, first in enumerate((108, 140, 156)):
            at[first + column] = 128 + 16 * n + column
        if column >= 12:
            at[160 + column] = 164 + column
    return at


def own_tiles(turn, column):
    late = (turn == 6) & (column >= 12)
    first = jnp.where(turn == 7, 124 + column, jnp.where(late, 164 + column, turn * 16 + column))
    second = jnp.where(turn == 7, 108, jnp.where(turn == 1, 140, jnp.where(turn == 5, 156, 160))) + column
    slot = jnp.where(turn == 7, 128, jnp.where(turn == 1, 144, jnp.where(turn == 5, 160, 164))) + column
    return first, turn * 16 + column, second, slot, (turn == 7) | (turn == 1) | (turn == 5) | late


STEPS = (4, 3, 5, 2, 6, 1, 7, 0)


def far_first(i):
    half = lax.div(i, 2)
    return (1 - half) * (2 + i) + half * (3 - i)


def frag_device(g):
    column = (g + 6) % 8
    return 8 * g + 2 * (column // 4) + column % 2, 2 * ((column // 2) % 2)


def gather_kernel(
    fock_hbm, pot_hbm, chem, bound, imp_hbm, pof_hbm, x_out,
    fock, pot, imp_flat, pof, m_src, m_all, pot_all, u_ref, s_in, s_fock, r_fock, s_pot, r_pot,
):
    ka = lax.axis_index("ka")
    orb = lax.axis_index("orb")
    barrier = pltpu.get_barrier_semaphore()
    for step in (1, 2, 3):
        pl.semaphore_signal(barrier, inc=1, device_id=(ka, (orb + step) % 4), device_id_type=MESH)
    loads = [
        pltpu.make_async_copy(source, target, s_in.at[n])
        for n, (source, target) in enumerate(
            ((fock_hbm, fock), (pot_hbm, pot), (imp_hbm, imp_flat), (pof_hbm, pof))
        )
    ]
    for load in loads:
        load.start()
    for load in loads:
        load.wait()
    m_src[...] = fock[0] + fock[1]
    pl.semaphore_wait(barrier, 3)
    for step in (2, 3, 1):
        to = (orb + step) % 4
        remote(pot, pot_all.at[orb], s_pot.at[step], r_pot.at[step], ka, to).start()
    for step in (2, 3, 1):
        to = (orb + step) % 4
        remote(m_src.at[to], m_all.at[orb], s_fock.at[step], r_fock.at[step], ka, to).start()
    pot_all[orb] = pot[...]
    m_all[orb] = m_src[orb]

    for step in (1, 2, 3):
        remote(pot, pot_all.at[(orb + 4 - step) % 4], s_pot.at[step], r_pot.at[step], ka, orb).wait_recv()
    slot_of = iota((N, 192), 0)
    col_of = iota((N, 192), 1)
    frag_of = slot_of // 48
    pot_of = jnp.zeros((N, 192), jnp.int32)
    for f in range(8):
        pot_of = jnp.where(frag_of == f, pof[f], pot_of)
    pick = ((col_of % 4 == pot_of) & (col_of // 4 == slot_of - 48 * frag_of)).astype(F32)
    stacked = contract(pick, pot_all[...].reshape(192, 48), ((1,), (0,)))
    spread = (iota((48, N), 1) % 48 == iota((48, N), 0)).astype(F32)
    wide = contract(stacked, spread, ((1,), (0,)))
    rows, cols = iota((N, N), 0), iota((N, N), 1)
    wide = jnp.where(rows // 48 == cols // 48, wide, 0.0)
    wide = 0.5 * (wide + wide.T)
    place = (rows == imp_flat[...].reshape(1, N)).astype(F32)
    u_ref[...] = contract(contract(place, wide, ((1,), (0,))), place, ((1,), (1,)))

    for step in (1, 2, 3):
        remote(
            m_src.at[0], m_all.at[(orb + 4 - step) % 4], s_fock.at[step], r_fock.at[step], ka, orb
        ).wait_recv()
    m = m_all[...].reshape(N, N)
    mt = m.T
    scale = 1.0 / bound[0]
    eye = (rows == cols).astype(F32)
    x_out[:, :N] = (0.5 * (m + mt) + u_ref[...] - chem[0] * eye) * scale
    x_out[:, N:] = (0.5 * (m - mt)) * scale
    for step in (1, 2, 3):
        remote(pot, pot_all.at[0], s_pot.at[step], r_pot.at[step], ka, orb).wait_send()
        remote(m_src.at[0], m_all.at[0], s_fock.at[step], r_fock.at[step], ka, orb).wait_send()


def main_kernel(
    x_in, imp_hbm, t_hi, t_lo, landing, f_in,
    imp_flat,
    x_ref, w_hi, w_lo, d_tiles, k_buf, o_buf, d0_buf, full, f_out,
    s_imp, entered, s_k, r_k, s_o, r_o, s_d0, r_d0, s_f, r_f,
):
    ka = lax.axis_index("ka")
    orb = lax.axis_index("orb")
    z, x, yl = ka // 8, (ka // 2) % 4, ka % 2
    yh, core = orb // 2, orb % 2
    me = ka * 4 + orb
    barrier = pltpu.get_barrier_semaphore()

    def greet(d, carry):
        plane = (ka + d // 4) % 8
        pl.semaphore_signal(barrier, inc=1, device_id=(8 * z + plane, (orb + d) % 4), device_id_type=MESH)
        return carry

    fetch = pltpu.make_async_copy(imp_hbm, imp_flat, s_imp)
    fetch.start()
    lax.fori_loop(1, 32, greet, 0)
    for step in range(1, 8):
        pl.semaphore_signal(barrier, inc=1, device_id=((ka + 8 * step) % 64, orb), device_id_type=MESH)

    x_ref[...] = x_in[...]
    rows, cols = iota((N, N), 0), iota((N, N), 1)
    eye = (rows == cols).astype(F32)
    for step in range(ITERS):
        hi, lo = split2(x_ref[...])
        for part, w in ((hi, w_hi), (lo, w_lo)):
            w[:N, :N] = part[:, :N]
            w[:N, N:] = part[:, N:]
            w[N:, :N] = -part[:, N:]
            w[N:, N:] = part[:, :N]
        s = dot3(hi, lo, w_hi[...], w_lo[...])
        s_hi, s_lo = split2(s)
        c = dot3(s_hi, s_lo, w_hi[...], w_lo[...])
        x_ref[...] = 1.5 * x_ref[...] - 0.5 * c
        if step == 0:
            fetch.wait()
            pl.semaphore_wait(barrier, 38)
            for hop in range(1, 8):
                pl.semaphore_signal(entered, inc=1, device_id=((ka + 8 * hop) % 64, orb), device_id_type=MESH)
    slot_of_tile = slots()
    values = (0.5 * eye - 0.5 * x_ref[:, :N], -0.5 * x_ref[:, N:])
    for n, (o, p) in enumerate(PAIRS):
        re, im = (pack(v[96 * o : 96 * o + 96, 96 * p : 96 * p + 96]).reshape(9, 8, 128) for v in values)
        for half in range(2):
            rows_at = slice(4 * half, 4 * half + 4)
            quads = jnp.concatenate([re[:, rows_at], im[:, rows_at]], axis=1)
            for t in range(9):
                d_tiles[slot_of_tile[18 * n + 9 * half + t]] = quads[t]

    column = x * 4 + yh * 2 + yl
    turn = lax.rem(z + 16 - column, 8)
    first, first_slot, second, second_slot, has_second = own_tiles(turn, column)
    own_tile = jnp.where(core == 1, first, second)
    own_slot = jnp.where(core == 1, first_slot, second_slot)
    has_tile = (core == 1) | has_second
    pl.semaphore_wait(entered, 7)

    def send_k(slot, to_ka, to_orb):
        remote(d_tiles.at[slot], k_buf.at[me], s_k, r_k, to_ka, to_orb).start()

    def column_at(e):
        to_x = lax.rem(x + far_first(lax.rem(e, 4)), 4)
        to_y = lax.rem(2 * yh + yl + far_first(lax.div(e, 4)), 4)
        to_yh, to_yl = lax.div(to_y, 2), lax.rem(to_y, 2)
        return to_x * 4 + to_yh * 2 + to_yl, to_x * 2 + to_yl, to_yh * 2

    def spread_first(e, carry):
        to_column, to_line, to_orb = column_at(e)
        for step in STEPS:
            to_z = lax.rem(z + step, 8)
            slot = lax.rem(to_z + 16 - to_column, 8) * 16 + to_column
            if step:
                send_k(slot, to_z * 8 + to_line, to_orb + 1)
            else:

                @pl.when((e < 15) | (core == 0))
                def _(slot=slot, to_z=to_z):
                    send_k(slot, to_z * 8 + to_line, to_orb + 1)

        return carry

    lax.fori_loop(0, 16, spread_first, 0)

    def spread_second(e, carry):
        to_column, to_line, to_orb = column_at(e)
        for n, to_turn in enumerate((7, 1, 5)):
            to_z = lax.rem(to_turn + to_column, 8)

            @pl.when((e < 15) | (core == 1) | (to_z != z))
            def _(n=n, to_z=to_z):
                send_k(128 + 16 * n + to_column, to_z * 8 + to_line, to_orb)

        return carry

    def spread_late(e, carry):
        place = lax.rem(e + column, 4)
        to_column = 12 + place
        to_z = lax.rem(6 + to_column, 8)

        @pl.when((to_column != column) | (core == 1) | (to_z != z))
        def _():
            send_k(164 + to_column, to_z * 8 + 6 + lax.rem(place, 2), 2 * lax.div(place, 2))

        return carry

    lax.fori_loop(0, 4, spread_late, 0)
    lax.fori_loop(0, 16, spread_second, 0)
    t_o, t_p = blocks_of(own_tile // 18)
    t_m = own_tile % 18
    mirrored = t_o != t_p
    to_self = (t_o == orb) | (t_p == orb)

    @pl.when(has_tile)
    def _():
        k_buf[me] = d_tiles[own_slot]
        wait_bytes(k_buf.at[pl.ds(0, K - 1)], r_k)
        k_rows = k_buf.reshape(K * 8, 128)
        o_rows = o_buf.reshape(2 * K * 8, 128)
        for s in range(4):
            both = [k_rows[pl.ds(c * 4 + s, K, stride=8), :] for c in range(2)]
            v_hi, v_lo = split2(jnp.concatenate(both, axis=1))
            res = dot3(t_hi[...], t_lo[...], v_hi, v_lo)
            cos_re, cos_im = res[:K, :128], res[:K, 128:]
            sin_re, sin_im = res[K:, :128], res[K:, 128:]
            o_rows[pl.ds(s, K, stride=8), :] = cos_re - sin_im
            o_rows[pl.ds(4 + s, K, stride=8), :] = cos_im + sin_re
            o_rows[pl.ds(K * 8 + s, K, stride=8), :] = cos_re + sin_im
            o_rows[pl.ds(K * 8 + 4 + s, K, stride=8), :] = sin_re - cos_im

        def send_d0(g, carry):
            to_ka, to_orb = frag_device(g)
            remote(o_buf.at[0, 0], d0_buf.at[own_tile], s_d0, r_d0, to_ka, to_orb).start()
            return carry

        lax.fori_loop(0, 8, send_d0, 0)

        def send_o(e, carry):
            to_x = lax.rem(x + far_first(lax.rem(e, 4)), 4)
            to_yl = lax.rem(yl + 1 - lax.div(e, 4), 2)
            to_line = to_x * 2 + to_yl

            def send_side(side, place, to_orb):
                for step in STEPS:
                    to_ka = lax.rem(z + step, 8) * 8 + to_line

                    def send(to_ka=to_ka):
                        cells_at = o_buf.at[side, pl.ds(4 * to_ka, 4)]
                        remote(cells_at, landing.at[place], s_o, r_o, to_ka, to_orb).start()

                    if step:
                        send()
                    else:
                        pl.when((e < 7) | (to_orb != orb))(send)

            send_side(0, t_p * 18 + t_m, t_o)

            @pl.when(mirrored)
            def _():
                send_side(1, t_o * 18 + t_m, t_p)

            return carry

        lax.fori_loop(0, 8, send_o, 0)

        @pl.when(t_o == orb)
        def _():
            landing[t_p * 18 + t_m] = o_buf[0, pl.ds(4 * ka, 4)]

        @pl.when(mirrored & (t_p == orb))
        def _():
            landing[t_o * 18 + t_m] = o_buf[1, pl.ds(4 * ka, 4)]

    f_o, f_half = z % 4, z // 4
    makes = (core == 0) & (column == (z + 6) % 8)

    @pl.when(makes)
    def _():
        imp = imp_flat[...].reshape(1, N)
        slots = [imp[:, 96 * o : 96 * o + 96] for o in range(4)]
        own_slots = slots[0]
        for o in range(1, 4):
            own_slots = jnp.where(f_o == o, slots[o], own_slots)
        own_slots = jnp.concatenate([own_slots, jnp.full((1, 32), -1, jnp.int32)], axis=1)
        wait_bytes(d0_buf, r_d0)
        chosen = (iota((N, 128), 0) == own_slots).astype(F32)
        left = iota((48, 128), 1) < 48
        for part in range(2):
            for n, (o, p) in enumerate(PAIRS):
                halves = [d0_buf[18 * n + 9 * h : 18 * n + 9 * h + 9, 4 * part : 4 * part + 4] for h in range(2)]
                block = unpack(jnp.concatenate(halves, axis=1).reshape(72, 128))
                full[96 * o : 96 * o + 96, 96 * p : 96 * p + 96] = block
                if o != p:
                    full[96 * p : 96 * p + 96, 96 * o : 96 * o + 96] = block.T if part == 0 else -block.T
            picked = contract(contract(chosen, full[...], ((0,), (0,))), chosen, ((1,), (0,)))
            f_out[part] = jnp.where(left, picked[:48], picked[48:96])

        def send_f(d, carry):
            to_ka = lax.rem(z + lax.rem(d * 3 + 4, 8), 8) * 8 + lax.rem(ka + lax.div(d, 8), 8)
            rows_at = pl.ds(pl.multiple_of(24 * f_half, 8), 24)
            remote(f_out.at[:, rows_at], f_in.at[:, rows_at], s_f, r_f, to_ka, f_o).start()
            return carry

        lax.fori_loop(0, 64, send_f, 0)

    wait_bytes(f_in, r_f)
    keeps = has_tile & to_self

    @pl.when(keeps)
    def _():
        wait_bytes(landing.at[pl.ds(0, 71)], r_o)

    @pl.when(jnp.logical_not(keeps))
    def _():
        wait_bytes(landing, r_o)

    @pl.when(has_tile)
    def _():
        wait_bytes(d_tiles.at[pl.ds(0, TILES - 1)], s_k)
        wait_bytes(d_tiles.at[pl.ds(0, 8)], s_d0)

    @pl.when(jnp.logical_not(has_tile))
    def _():
        wait_bytes(d_tiles, s_k)

    for side, sent, fewer in (
        (mirrored, o_buf, o_buf.at[:, pl.ds(0, K - 2)]),
        (jnp.logical_not(mirrored), o_buf.at[0], o_buf.at[0, pl.ds(0, K - 4)]),
    ):

        @pl.when(has_tile & side & to_self)
        def _(fewer=fewer):
            wait_bytes(fewer, s_o)

        @pl.when(has_tile & side & jnp.logical_not(to_self))
        def _(sent=sent):
            wait_bytes(sent, s_o)

    @pl.when(makes)
    def _():
        wait_bytes(o_buf.at[:, pl.ds(0, 192)], s_f)


def store_kernel(landing, f_in, out, frag, buf, sem):
    own = lax.axis_index("orb")
    stores = [
        [pltpu.make_async_copy(buf.at[c, r], out.at[c, r], sem.at[c, r]) for r in range(4)] for c in range(2)
    ]
    for place in range(4):

        @pl.when(own == place)
        def _(place=place):
            for r in range(4):
                for c in range(2):
                    blocks = []
                    for q in range(4):
                        halves = [
                            landing[18 * q + 9 * h : 18 * q + 9 * h + 9, r, 4 * c : 4 * c + 4] for h in range(2)
                        ]
                        block = unpack(jnp.concatenate(halves, axis=1).reshape(72, 128))
                        blocks.append(block if place <= q else block.T)
                    buf[c, r] = jnp.concatenate(blocks, axis=1)
                    stores[c][r].start()

    for part in range(2):
        for f in range(2):
            frag[part, f] = f_in[part, :, 48 * f : 48 * f + 48]
    for store in stores[0] + stores[1]:
        store.wait()


def tables():
    grid = np.outer(np.arange(K), np.arange(K)) % K
    angle = grid * (2.0 * math.pi / K)
    c, s = np.cos(angle) / K, np.sin(angle) / K
    full = np.concatenate([c, s]).astype(np.float32)
    hi = full.astype(jnp.bfloat16)
    lo = (full - hi.astype(np.float32)).astype(jnp.bfloat16)
    return hi, lo


def per_device(fock, potential, chem_potential, spectral_bound, impurity_orbitals, potential_of):
    t_hi, t_lo = tables()
    vmem = pl.BlockSpec(memory_space=pltpu.VMEM)
    smem = pl.BlockSpec(memory_space=pltpu.SMEM)
    hbm = pl.BlockSpec(memory_space=pltpu.HBM)
    dma = pltpu.SemaphoreType.DMA
    pot = potential.transpose(1, 0, 2).reshape(48, 48)
    imp = pltpu.with_memory_space_constraint(impurity_orbitals, pltpu.HBM)
    start = pl.pallas_call(
        gather_kernel,
        name="gather",
        out_shape=jax.ShapeDtypeStruct((N, 2 * N), F32),
        in_specs=[hbm, hbm, smem, smem, hbm, hbm],
        out_specs=vmem,
        scratch_shapes=[
            pltpu.VMEM((2, 4, 96, N), F32),
            pltpu.VMEM((48, 48), F32),
            pltpu.VMEM((N,), jnp.int32),
            pltpu.SMEM((8,), jnp.int32),
            pltpu.VMEM((4, 96, N), F32),
            pltpu.VMEM((4, 96, N), F32),
            pltpu.VMEM((4, 48, 48), F32),
            pltpu.VMEM((N, N), F32),
            dma((4,)), dma((4,)), dma((4,)), dma((4,)), dma((4,)),
        ],
        compiler_params=pltpu.CompilerParams(
            has_side_effects=True, collective_id=0, vmem_limit_bytes=40 << 20
        ),
    )(
        pltpu.with_memory_space_constraint(fock, pltpu.HBM),
        pltpu.with_memory_space_constraint(pot, pltpu.HBM),
        chem_potential,
        spectral_bound,
        imp,
        pltpu.with_memory_space_constraint(potential_of, pltpu.HBM),
    )
    landing, f_in = pl.pallas_call(
        main_kernel,
        name="transform",
        out_shape=(
            jax.ShapeDtypeStruct((72, 4, 8, 128), F32),
            jax.ShapeDtypeStruct((2, 48, 128), F32),
        ),
        in_specs=[vmem, hbm, vmem, vmem],
        out_specs=(vmem, vmem),
        scratch_shapes=[
            pltpu.VMEM((N,), jnp.int32),
            pltpu.VMEM((N, 2 * N), F32),
            pltpu.VMEM((2 * N, 2 * N), BF16),
            pltpu.VMEM((2 * N, 2 * N), BF16),
            pltpu.VMEM((TILES, 8, 128), F32),
            pltpu.VMEM((K, 8, 128), F32),
            pltpu.VMEM((2, K, 8, 128), F32),
            pltpu.VMEM((TILES, 8, 128), F32),
            pltpu.VMEM((N, N), F32),
            pltpu.VMEM((2, 48, 128), F32),
            dma,
            pltpu.SemaphoreType.REGULAR,
            dma, dma, dma, dma, dma, dma, dma, dma,
        ],
        compiler_params=pltpu.CompilerParams(
            has_side_effects=True, collective_id=1, vmem_limit_bytes=48 << 20
        ),
    )(start, imp, jnp.asarray(t_hi), jnp.asarray(t_lo))
    return pl.pallas_call(
        store_kernel,
        name="store",
        out_shape=(
            jax.ShapeDtypeStruct((2, 4, 96, N), F32),
            jax.ShapeDtypeStruct((2, 2, 48, 48), F32),
        ),
        in_specs=[vmem, vmem],
        out_specs=(hbm, vmem),
        scratch_shapes=[pltpu.VMEM((2, 4, 96, N), F32), dma((2, 4))],
        compiler_params=pltpu.CompilerParams(vmem_limit_bytes=8 << 20),
    )(landing, f_in)


def solution(mesh):
    return jax.shard_map(
        per_device,
        mesh=mesh,
        in_specs=(P(None, "ka", "orb", None), P(None, "orb", None), P(), P(), P(), P()),
        out_specs=(P(None, "ka", "orb", None), P(None, "orb", None, None)),
        check_vma=False,
    )
```

```python
import functools
import math

import jax
import jax.numpy as jnp
import numpy as np
from jax import lax
from jax.experimental import pallas as pl
from jax.experimental.pallas import tpu as pltpu
from jax.sharding import PartitionSpec as P

ITERS = 2
N = 384
K = 256
F32 = jnp.float32
BF16 = jnp.bfloat16
MESH = pl.DeviceIdType.MESH


def split2(x):
    hi = x.astype(BF16)
    return hi, (x - hi.astype(F32)).astype(BF16)


def dot(a, b):
    return jnp.dot(a, b, preferred_element_type=F32)


def dot3(a_hi, a_lo, b_hi, b_lo):
    return dot(a_hi, b_hi) + (dot(a_hi, b_lo) + dot(a_lo, b_hi))


def contract(a, b, dims):
    return lax.dot_general(
        a, b, (dims, ((), ())), precision=lax.Precision.HIGHEST, preferred_element_type=F32
    )


def iota(shape, dim):
    return lax.broadcasted_iota(jnp.int32, shape, dim)


def remote(src, dst, send, recv, ka, orb):
    return pltpu.make_async_remote_copy(
        src_ref=src, dst_ref=dst, send_sem=send, recv_sem=recv, device_id=(ka, orb), device_id_type=MESH
    )


def wait_bytes(ref, sem):
    pltpu.make_async_copy(ref, ref, sem).wait()


PAIRS = ((0, 1), (0, 2), (0, 3), (1, 2), (1, 3), (2, 3), (0, 0), (1, 1), (2, 2), (3, 3))
TILES = 18 * len(PAIRS)


def pack(block):
    a, b, c, d = (block[24 * n : 24 * n + 24] for n in range(4))
    return jnp.concatenate(
        [
            jnp.concatenate([a, b[:, :32]], axis=1),
            jnp.concatenate([b[:, 32:], c[:, :64]], axis=1),
            jnp.concatenate([c[:, 64:], d], axis=1),
        ],
        axis=0,
    )


def unpack(packed):
    p, q, r = (packed[24 * n : 24 * n + 24] for n in range(3))
    return jnp.concatenate(
        [
            p[:, :96],
            jnp.concatenate([p[:, 96:], q[:, :64]], axis=1),
            jnp.concatenate([q[:, 64:], r[:, :32]], axis=1),
            r[:, 32:],
        ],
        axis=0,
    )


def blocks_of(pair):
    late, last = (pair >= 3).astype(jnp.int32), (pair >= 5).astype(jnp.int32)
    diagonal = pair >= 6
    return (
        jnp.where(diagonal, pair - 6, late + last),
        jnp.where(diagonal, pair - 6, pair + 1 - 2 * late - last),
    )


def slots():
    at = {}
    for column in range(16):
        for turn in range(8):
            tile = turn * 16 + column
            if turn == 7:
                tile = 124 + column
            elif turn == 6 and column >= 12:
                tile = 164 + column
            at[tile] = turn * 16 + column
        for n, first in enumerate((108, 140, 156)):
            at[first + column] = 128 + 16 * n + column
        if column >= 12:
            at[160 + column] = 164 + column
    return at


def own_tiles(turn, column):
    late = (turn == 6) & (column >= 12)
    first = jnp.where(turn == 7, 124 + column, jnp.where(late, 164 + column, turn * 16 + column))
    second = jnp.where(turn == 7, 108, jnp.where(turn == 1, 140, jnp.where(turn == 5, 156, 160))) + column
    slot = jnp.where(turn == 7, 128, jnp.where(turn == 1, 144, jnp.where(turn == 5, 160, 164))) + column
    return first, turn * 16 + column, second, slot, (turn == 7) | (turn == 1) | (turn == 5) | late


STEPS = (4, 3, 5, 2, 6, 1, 7, 0)


def far_first(i):
    half = lax.div(i, 2)
    return (1 - half) * (2 + i) + half * (3 - i)


def frag_device(g):
    z = lax.rem(g + 3, 8)
    return 8 * z + 2 * lax.div(g, 4) + lax.rem(g, 2), 2 * lax.rem(lax.div(g, 2), 2)


def gather_kernel(
    fock_hbm, pot_hbm, chem, bound, imp_hbm, pof_hbm, x_out,
    fock, pot, imp_flat, pof, m_src, m_all, pot_all, u_ref, s_in, s_fock, r_fock, s_pot, r_pot,
):
    ka = lax.axis_index("ka")
    orb = lax.axis_index("orb")
    barrier = pltpu.get_barrier_semaphore()
    for step in (1, 2, 3):
        pl.semaphore_signal(barrier, inc=1, device_id=(ka, (orb + step) % 4), device_id_type=MESH)
    loads = [
        pltpu.make_async_copy(source, target, s_in.at[n])
        for n, (source, target) in enumerate(
            ((fock_hbm, fock), (pot_hbm, pot), (imp_hbm, imp_flat), (pof_hbm, pof))
        )
    ]
    for load in loads:
        load.start()
    for load in loads:
        load.wait()
    m_src[...] = fock[0] + fock[1]
    pl.semaphore_wait(barrier, 3)
    for step in (2, 3, 1):
        to = (orb + step) % 4
        remote(pot, pot_all.at[orb], s_pot.at[step], r_pot.at[step], ka, to).start()
    for step in (2, 3, 1):
        to = (orb + step) % 4
        remote(m_src.at[to], m_all.at[orb], s_fock.at[step], r_fock.at[step], ka, to).start()
    pot_all[orb] = pot[...]
    m_all[orb] = m_src[orb]

    for step in (1, 2, 3):
        remote(pot, pot_all.at[(orb + 4 - step) % 4], s_pot.at[step], r_pot.at[step], ka, orb).wait_recv()
    slot_of = iota((N, 192), 0)
    col_of = iota((N, 192), 1)
    frag_of = slot_of // 48
    pot_of = jnp.zeros((N, 192), jnp.int32)
    for f in range(8):
        pot_of = jnp.where(frag_of == f, pof[f], pot_of)
    pick = ((col_of % 4 == pot_of) & (col_of // 4 == slot_of - 48 * frag_of)).astype(F32)
    stacked = contract(pick, pot_all[...].reshape(192, 48), ((1,), (0,)))
    spread = (iota((48, N), 1) % 48 == iota((48, N), 0)).astype(F32)
    wide = contract(stacked, spread, ((1,), (0,)))
    rows, cols = iota((N, N), 0), iota((N, N), 1)
    wide = jnp.where(rows // 48 == cols // 48, wide, 0.0)
    wide = 0.5 * (wide + wide.T)
    place = (rows == imp_flat[...].reshape(1, N)).astype(F32)
    u_ref[...] = contract(contract(place, wide, ((1,), (0,))), place, ((1,), (1,)))

    for step in (1, 2, 3):
        remote(
            m_src.at[0], m_all.at[(orb + 4 - step) % 4], s_fock.at[step], r_fock.at[step], ka, orb
        ).wait_recv()
    m = m_all[...].reshape(N, N)
    mt = m.T
    scale = 1.0 / bound[0]
    eye = (rows == cols).astype(F32)
    x_out[:, :N] = (0.5 * (m + mt) + u_ref[...] - chem[0] * eye) * scale
    x_out[:, N:] = (0.5 * (m - mt)) * scale
    for step in (1, 2, 3):
        remote(pot, pot_all.at[0], s_pot.at[step], r_pot.at[step], ka, orb).wait_send()
        remote(m_src.at[0], m_all.at[0], s_fock.at[step], r_fock.at[step], ka, orb).wait_send()


def main_kernel(
    x_in, imp_hbm, t_hi, t_lo, landing, f_in,
    imp_flat,
    x_ref, w_hi, w_lo, d_tiles, k_buf, o_buf, d0_buf, full, f_out,
    s_imp, entered, s_k, r_k, s_o, r_o, s_d0, r_d0, s_f, r_f,
):
    ka = lax.axis_index("ka")
    orb = lax.axis_index("orb")
    z, x, yl = ka // 8, (ka // 2) % 4, ka % 2
    yh, core = orb // 2, orb % 2
    me = ka * 4 + orb
    barrier = pltpu.get_barrier_semaphore()

    def greet(d, carry):
        plane = (ka + d // 4) % 8
        pl.semaphore_signal(barrier, inc=1, device_id=(8 * z + plane, (orb + d) % 4), device_id_type=MESH)
        return carry

    fetch = pltpu.make_async_copy(imp_hbm, imp_flat, s_imp)
    fetch.start()
    lax.fori_loop(1, 32, greet, 0)
    for step in range(1, 8):
        pl.semaphore_signal(barrier, inc=1, device_id=((ka + 8 * step) % 64, orb), device_id_type=MESH)

    x_ref[...] = x_in[...]
    rows, cols = iota((N, N), 0), iota((N, N), 1)
    eye = (rows == cols).astype(F32)
    for step in range(ITERS):
        hi, lo = split2(x_ref[...])
        for part, w in ((hi, w_hi), (lo, w_lo)):
            w[:N, :N] = part[:, :N]
            w[:N, N:] = part[:, N:]
            w[N:, :N] = -part[:, N:]
            w[N:, N:] = part[:, :N]
        s = dot3(hi, lo, w_hi[...], w_lo[...])
        s_hi, s_lo = split2(s)
        c = dot3(s_hi, s_lo, w_hi[...], w_lo[...])
        x_ref[...] = 1.5 * x_ref[...] - 0.5 * c
        if step == 0:
            fetch.wait()
            pl.semaphore_wait(barrier, 38)
            for hop in range(1, 8):
                pl.semaphore_signal(entered, inc=1, device_id=((ka + 8 * hop) % 64, orb), device_id_type=MESH)
    slot_of_tile = slots()
    values = (0.5 * eye - 0.5 * x_ref[:, :N], -0.5 * x_ref[:, N:])
    for n, (o, p) in enumerate(PAIRS):
        re, im = (pack(v[96 * o : 96 * o + 96, 96 * p : 96 * p + 96]).reshape(9, 8, 128) for v in values)
        for half in range(2):
            rows_at = slice(4 * half, 4 * half + 4)
            quads = jnp.concatenate([re[:, rows_at], im[:, rows_at]], axis=1)
            for t in range(9):
                d_tiles[slot_of_tile[18 * n + 9 * half + t]] = quads[t]

    column = x * 4 + yh * 2 + yl
    turn = lax.rem(z + 16 - column, 8)
    first, first_slot, second, second_slot, has_second = own_tiles(turn, column)
    own_tile = jnp.where(core == 1, first, second)
    own_slot = jnp.where(core == 1, first_slot, second_slot)
    has_tile = (core == 1) | has_second
    pl.semaphore_wait(entered, 7)

    def send_k(slot, to_ka, to_orb):
        remote(d_tiles.at[slot], k_buf.at[me], s_k, r_k, to_ka, to_orb).start()

    def column_at(e):
        to_x = lax.rem(x + far_first(lax.rem(e, 4)), 4)
        to_y = lax.rem(2 * yh + yl + far_first(lax.div(e, 4)), 4)
        to_yh, to_yl = lax.div(to_y, 2), lax.rem(to_y, 2)
        return to_x * 4 + to_yh * 2 + to_yl, to_x * 2 + to_yl, to_yh * 2

    def spread_first(e, carry):
        to_column, to_line, to_orb = column_at(e)
        for step in STEPS:
            to_z = lax.rem(z + step, 8)
            slot = lax.rem(to_z + 16 - to_column, 8) * 16 + to_column
            if step:
                send_k(slot, to_z * 8 + to_line, to_orb + 1)
            else:

                @pl.when((e < 15) | (core == 0))
                def _(slot=slot, to_z=to_z):
                    send_k(slot, to_z * 8 + to_line, to_orb + 1)

        return carry

    lax.fori_loop(0, 16, spread_first, 0)

    def spread_second(e, carry):
        to_column, to_line, to_orb = column_at(e)
        for n, to_turn in enumerate((7, 1, 5)):
            to_z = lax.rem(to_turn + to_column, 8)

            @pl.when((e < 15) | (core == 1) | (to_z != z))
            def _(n=n, to_z=to_z):
                send_k(128 + 16 * n + to_column, to_z * 8 + to_line, to_orb)

        return carry

    def spread_late(e, carry):
        place = lax.rem(e + column, 4)
        to_column = 12 + place
        to_z = lax.rem(6 + to_column, 8)

        @pl.when((to_column != column) | (core == 1) | (to_z != z))
        def _():
            send_k(164 + to_column, to_z * 8 + 6 + lax.rem(place, 2), 2 * lax.div(place, 2))

        return carry

    lax.fori_loop(0, 4, spread_late, 0)
    lax.fori_loop(0, 16, spread_second, 0)
    t_o, t_p = blocks_of(own_tile // 18)
    t_m = own_tile % 18
    mirrored = t_o != t_p
    to_self = (t_o == orb) | (t_p == orb)

    @pl.when(has_tile)
    def _():
        k_buf[me] = d_tiles[own_slot]
        wait_bytes(k_buf.at[pl.ds(0, K - 1)], r_k)
        k_rows = k_buf.reshape(K * 8, 128)
        o_rows = o_buf.reshape(2 * K * 8, 128)
        for s in range(4):
            both = [k_rows[pl.ds(c * 4 + s, K, stride=8), :] for c in range(2)]
            v_hi, v_lo = split2(jnp.concatenate(both, axis=1))
            res = dot3(t_hi[...], t_lo[...], v_hi, v_lo)
            cos_re, cos_im = res[:K, :128], res[:K, 128:]
            sin_re, sin_im = res[K:, :128], res[K:, 128:]
            o_rows[pl.ds(s, K, stride=8), :] = cos_re - sin_im
            o_rows[pl.ds(4 + s, K, stride=8), :] = cos_im + sin_re
            o_rows[pl.ds(K * 8 + s, K, stride=8), :] = cos_re + sin_im
            o_rows[pl.ds(K * 8 + 4 + s, K, stride=8), :] = sin_re - cos_im

        def send_d0(g, carry):
            to_ka, to_orb = frag_device(g)
            remote(o_buf.at[0, 0], d0_buf.at[own_tile], s_d0, r_d0, to_ka, to_orb).start()
            return carry

        lax.fori_loop(0, 12, send_d0, 0)

        def send_o(e, carry):
            to_x = lax.rem(x + far_first(lax.rem(e, 4)), 4)
            to_yl = lax.rem(yl + 1 - lax.div(e, 4), 2)
            to_line = to_x * 2 + to_yl

            def send_side(side, place, to_orb):
                for step in STEPS:
                    to_ka = lax.rem(z + step, 8) * 8 + to_line

                    def send(to_ka=to_ka):
                        cells_at = o_buf.at[side, pl.ds(4 * to_ka, 4)]
                        remote(cells_at, landing.at[place], s_o, r_o, to_ka, to_orb).start()

                    if step:
                        send()
                    else:
                        pl.when((e < 7) | (to_orb != orb))(send)

            send_side(0, t_p * 18 + t_m, t_o)

            @pl.when(mirrored)
            def _():
                send_side(1, t_o * 18 + t_m, t_p)

            return carry

        lax.fori_loop(0, 8, send_o, 0)

        @pl.when(t_o == orb)
        def _():
            landing[t_p * 18 + t_m] = o_buf[0, pl.ds(4 * ka, 4)]

        @pl.when(mirrored & (t_p == orb))
        def _():
            landing[t_o * 18 + t_m] = o_buf[1, pl.ds(4 * ka, 4)]

    f_o, f_part = lax.rem(column + 1, 4), lax.div(column, 4)
    makes = (core == 0) & (turn == 3) & (column < 12)

    @pl.when(makes)
    def _():
        imp = imp_flat[...].reshape(1, N)
        slots = [imp[:, 96 * o : 96 * o + 96] for o in range(4)]
        own_slots = slots[0]
        for o in range(1, 4):
            own_slots = jnp.where(f_o == o, slots[o], own_slots)
        own_slots = jnp.concatenate([own_slots, jnp.full((1, 32), -1, jnp.int32)], axis=1)
        wait_bytes(d0_buf, r_d0)
        chosen = (iota((N, 128), 0) == own_slots).astype(F32)
        left = iota((48, 128), 1) < 48
        for part in range(2):
            for n, (o, p) in enumerate(PAIRS):
                halves = [d0_buf[18 * n + 9 * h : 18 * n + 9 * h + 9, 4 * part : 4 * part + 4] for h in range(2)]
                block = unpack(jnp.concatenate(halves, axis=1).reshape(72, 128))
                full[96 * o : 96 * o + 96, 96 * p : 96 * p + 96] = block
                if o != p:
                    full[96 * p : 96 * p + 96, 96 * o : 96 * o + 96] = block.T if part == 0 else -block.T
            picked = contract(contract(chosen, full[...], ((0,), (0,))), chosen, ((1,), (0,)))
            f_out[part] = jnp.where(left, picked[:48], picked[48:96])

        def send_f(d, carry):
            to_ka = lax.rem(z + lax.rem(d * 3 + 4, 8), 8) * 8 + lax.rem(ka + lax.div(d, 8), 8)
            rows_at = pl.ds(pl.multiple_of(16 * f_part, 8), 16)
            remote(f_out.at[:, rows_at], f_in.at[:, rows_at], s_f, r_f, to_ka, f_o).start()
            return carry

        lax.fori_loop(0, 64, send_f, 0)

    wait_bytes(f_in, r_f)
    keeps = has_tile & to_self

    @pl.when(keeps)
    def _():
        wait_bytes(landing.at[pl.ds(0, 71)], r_o)

    @pl.when(jnp.logical_not(keeps))
    def _():
        wait_bytes(landing, r_o)

    @pl.when(has_tile)
    def _():
        wait_bytes(d_tiles.at[pl.ds(0, TILES - 1)], s_k)
        wait_bytes(d_tiles.at[pl.ds(0, 12)], s_d0)

    @pl.when(jnp.logical_not(has_tile))
    def _():
        wait_bytes(d_tiles, s_k)

    for side, sent, fewer in (
        (mirrored, o_buf, o_buf.at[:, pl.ds(0, K - 2)]),
        (jnp.logical_not(mirrored), o_buf.at[0], o_buf.at[0, pl.ds(0, K - 4)]),
    ):

        @pl.when(has_tile & side & to_self)
        def _(fewer=fewer):
            wait_bytes(fewer, s_o)

        @pl.when(has_tile & side & jnp.logical_not(to_self))
        def _(sent=sent):
            wait_bytes(sent, s_o)

    @pl.when(makes)
    def _():
        wait_bytes(k_buf, s_f)


def store_kernel(landing, f_in, out, frag, buf, sem):
    own = lax.axis_index("orb")
    stores = [
        [pltpu.make_async_copy(buf.at[c, r], out.at[c, r], sem.at[c, r]) for r in range(4)] for c in range(2)
    ]
    for place in range(4):

        @pl.when(own == place)
        def _(place=place):
            for r in range(4):
                for c in range(2):
                    blocks = []
                    for q in range(4):
                        halves = [
                            landing[18 * q + 9 * h : 18 * q + 9 * h + 9, r, 4 * c : 4 * c + 4] for h in range(2)
                        ]
                        block = unpack(jnp.concatenate(halves, axis=1).reshape(72, 128))
                        blocks.append(block if place <= q else block.T)
                    buf[c, r] = jnp.concatenate(blocks, axis=1)
                    stores[c][r].start()

    for part in range(2):
        for f in range(2):
            frag[part, f] = f_in[part, :, 48 * f : 48 * f + 48]
    for store in stores[0] + stores[1]:
        store.wait()


def tables():
    grid = np.outer(np.arange(K), np.arange(K)) % K
    angle = grid * (2.0 * math.pi / K)
    c, s = np.cos(angle) / K, np.sin(angle) / K
    full = np.concatenate([c, s]).astype(np.float32)
    hi = full.astype(jnp.bfloat16)
    lo = (full - hi.astype(np.float32)).astype(jnp.bfloat16)
    return hi, lo


def per_device(fock, potential, chem_potential, spectral_bound, impurity_orbitals, potential_of):
    t_hi, t_lo = tables()
    vmem = pl.BlockSpec(memory_space=pltpu.VMEM)
    smem = pl.BlockSpec(memory_space=pltpu.SMEM)
    hbm = pl.BlockSpec(memory_space=pltpu.HBM)
    dma = pltpu.SemaphoreType.DMA
    pot = potential.transpose(1, 0, 2).reshape(48, 48)
    imp = pltpu.with_memory_space_constraint(impurity_orbitals, pltpu.HBM)
    start = pl.pallas_call(
        gather_kernel,
        name="gather",
        out_shape=jax.ShapeDtypeStruct((N, 2 * N), F32),
        in_specs=[hbm, hbm, smem, smem, hbm, hbm],
        out_specs=vmem,
        scratch_shapes=[
            pltpu.VMEM((2, 4, 96, N), F32),
            pltpu.VMEM((48, 48), F32),
            pltpu.VMEM((N,), jnp.int32),
            pltpu.SMEM((8,), jnp.int32),
            pltpu.VMEM((4, 96, N), F32),
            pltpu.VMEM((4, 96, N), F32),
            pltpu.VMEM((4, 48, 48), F32),
            pltpu.VMEM((N, N), F32),
            dma((4,)), dma((4,)), dma((4,)), dma((4,)), dma((4,)),
        ],
        compiler_params=pltpu.CompilerParams(
            has_side_effects=True, collective_id=0, vmem_limit_bytes=40 << 20
        ),
    )(
        pltpu.with_memory_space_constraint(fock, pltpu.HBM),
        pltpu.with_memory_space_constraint(pot, pltpu.HBM),
        chem_potential,
        spectral_bound,
        imp,
        pltpu.with_memory_space_constraint(potential_of, pltpu.HBM),
    )
    landing, f_in = pl.pallas_call(
        main_kernel,
        name="transform",
        out_shape=(
            jax.ShapeDtypeStruct((72, 4, 8, 128), F32),
            jax.ShapeDtypeStruct((2, 48, 128), F32),
        ),
        in_specs=[vmem, hbm, vmem, vmem],
        out_specs=(vmem, vmem),
        scratch_shapes=[
            pltpu.VMEM((N,), jnp.int32),
            pltpu.VMEM((N, 2 * N), F32),
            pltpu.VMEM((2 * N, 2 * N), BF16),
            pltpu.VMEM((2 * N, 2 * N), BF16),
            pltpu.VMEM((TILES, 8, 128), F32),
            pltpu.VMEM((K, 8, 128), F32),
            pltpu.VMEM((2, K, 8, 128), F32),
            pltpu.VMEM((TILES, 8, 128), F32),
            pltpu.VMEM((N, N), F32),
            pltpu.VMEM((2, 48, 128), F32),
            dma,
            pltpu.SemaphoreType.REGULAR,
            dma, dma, dma, dma, dma, dma, dma, dma,
        ],
        compiler_params=pltpu.CompilerParams(
            has_side_effects=True, collective_id=1, vmem_limit_bytes=48 << 20
        ),
    )(start, imp, jnp.asarray(t_hi), jnp.asarray(t_lo))
    return pl.pallas_call(
        store_kernel,
        name="store",
        out_shape=(
            jax.ShapeDtypeStruct((2, 4, 96, N), F32),
            jax.ShapeDtypeStruct((2, 2, 48, 48), F32),
        ),
        in_specs=[vmem, vmem],
        out_specs=(hbm, vmem),
        scratch_shapes=[pltpu.VMEM((2, 4, 96, N), F32), dma((2, 4))],
        compiler_params=pltpu.CompilerParams(vmem_limit_bytes=8 << 20),
    )(landing, f_in)


def solution(mesh):
    return jax.shard_map(
        per_device,
        mesh=mesh,
        in_specs=(P(None, "ka", "orb", None), P(None, "orb", None), P(), P(), P(), P()),
        out_specs=(P(None, "ka", "orb", None), P(None, "orb", None, None)),
        check_vma=False,
    )
```

```python
import functools
import math

import jax
import jax.numpy as jnp
import numpy as np
from jax import lax
from jax.experimental import pallas as pl
from jax.experimental.pallas import tpu as pltpu
from jax.sharding import PartitionSpec as P

ITERS = 2
N = 384
K = 256
F32 = jnp.float32
BF16 = jnp.bfloat16
MESH = pl.DeviceIdType.MESH


def split2(x):
    hi = x.astype(BF16)
    return hi, (x - hi.astype(F32)).astype(BF16)


def dot(a, b):
    return jnp.dot(a, b, preferred_element_type=F32)


def dot3(a_hi, a_lo, b_hi, b_lo):
    return dot(a_hi, b_hi) + (dot(a_hi, b_lo) + dot(a_lo, b_hi))


def contract(a, b, dims):
    return lax.dot_general(
        a, b, (dims, ((), ())), precision=lax.Precision.HIGHEST, preferred_element_type=F32
    )


def iota(shape, dim):
    return lax.broadcasted_iota(jnp.int32, shape, dim)


def remote(src, dst, send, recv, ka, orb):
    return pltpu.make_async_remote_copy(
        src_ref=src, dst_ref=dst, send_sem=send, recv_sem=recv, device_id=(ka, orb), device_id_type=MESH
    )


def wait_bytes(ref, sem):
    pltpu.make_async_copy(ref, ref, sem).wait()


PAIRS = ((0, 1), (0, 2), (0, 3), (1, 2), (1, 3), (2, 3), (0, 0), (1, 1), (2, 2), (3, 3))
TILES = 18 * len(PAIRS)


def pack(block):
    a, b, c, d = (block[24 * n : 24 * n + 24] for n in range(4))
    return jnp.concatenate(
        [
            jnp.concatenate([a, b[:, :32]], axis=1),
            jnp.concatenate([b[:, 32:], c[:, :64]], axis=1),
            jnp.concatenate([c[:, 64:], d], axis=1),
        ],
        axis=0,
    )


def unpack(packed):
    p, q, r = (packed[24 * n : 24 * n + 24] for n in range(3))
    return jnp.concatenate(
        [
            p[:, :96],
            jnp.concatenate([p[:, 96:], q[:, :64]], axis=1),
            jnp.concatenate([q[:, 64:], r[:, :32]], axis=1),
            r[:, 32:],
        ],
        axis=0,
    )


def blocks_of(pair):
    late, last = (pair >= 3).astype(jnp.int32), (pair >= 5).astype(jnp.int32)
    diagonal = pair >= 6
    return (
        jnp.where(diagonal, pair - 6, late + last),
        jnp.where(diagonal, pair - 6, pair + 1 - 2 * late - last),
    )


def slots():
    at = {}
    for column in range(16):
        for turn in range(8):
            tile = turn * 16 + column
            if turn == 7:
                tile = 124 + column
            elif turn == 6 and column >= 12:
                tile = 164 + column
            at[tile] = turn * 16 + column
        for n, first in enumerate((108, 140, 156)):
            at[first + column] = 128 + 16 * n + column
        if column >= 12:
            at[160 + column] = 164 + column
    return at


def own_tiles(turn, column):
    late = (turn == 6) & (column >= 12)
    first = jnp.where(turn == 7, 124 + column, jnp.where(late, 164 + column, turn * 16 + column))
    second = jnp.where(turn == 7, 108, jnp.where(turn == 1, 140, jnp.where(turn == 5, 156, 160))) + column
    slot = jnp.where(turn == 7, 128, jnp.where(turn == 1, 144, jnp.where(turn == 5, 160, 164))) + column
    return first, turn * 16 + column, second, slot, (turn == 7) | (turn == 1) | (turn == 5) | late


STEPS = (4, 3, 5, 2, 6, 1, 7, 0)


def far_first(i):
    half = lax.div(i, 2)
    return (1 - half) * (2 + i) + half * (3 - i)


def frag_device(g):
    z = lax.rem(g + 3, 8)
    return 8 * z + 2 * lax.div(g, 4) + lax.rem(g, 2), 2 * lax.rem(lax.div(g, 2), 2)


def gather_kernel(
    fock_hbm, pot_hbm, chem, bound, imp_hbm, pof_hbm, x_out,
    fock, pot, imp_flat, pof, m_src, m_all, pot_all, u_ref, s_in, s_fock, r_fock, s_pot, r_pot,
):
    ka = lax.axis_index("ka")
    orb = lax.axis_index("orb")
    barrier = pltpu.get_barrier_semaphore()
    for step in (1, 2, 3):
        pl.semaphore_signal(barrier, inc=1, device_id=(ka, (orb + step) % 4), device_id_type=MESH)
    loads = [
        pltpu.make_async_copy(source, target, s_in.at[n])
        for n, (source, target) in enumerate(
            ((pot_hbm, pot), (imp_hbm, imp_flat), (pof_hbm, pof))
        )
    ]
    parts = {}
    for n, step in enumerate((2, 3, 1, 0)):
        to = (orb + step) % 4
        parts[step] = pltpu.make_async_copy(fock_hbm.at[:, to], fock.at[:, to], s_in.at[3 + n])
        parts[step].start()
    for load in loads:
        load.start()
    def add(step):
        to = (orb + step) % 4
        parts[step].wait()
        m_src[to] = fock[0, to] + fock[1, to]

    add(2)
    pl.semaphore_wait(barrier, 3)
    for step in (2, 3, 1):
        if step != 2:
            add(step)
        to = (orb + step) % 4
        remote(m_src.at[to], m_all.at[orb], s_fock.at[step], r_fock.at[step], ka, to).start()
    for load in loads:
        load.wait()
    for step in (2, 3, 1):
        remote(pot, pot_all.at[orb], s_pot.at[step], r_pot.at[step], ka, (orb + step) % 4).start()
    add(0)
    pot_all[orb] = pot[...]
    m_all[orb] = m_src[orb]

    for step in (1, 2, 3):
        remote(pot, pot_all.at[(orb + 4 - step) % 4], s_pot.at[step], r_pot.at[step], ka, orb).wait_recv()
    slot_of = iota((N, 192), 0)
    col_of = iota((N, 192), 1)
    frag_of = slot_of // 48
    pot_of = jnp.zeros((N, 192), jnp.int32)
    for f in range(8):
        pot_of = jnp.where(frag_of == f, pof[f], pot_of)
    pick = ((col_of % 4 == pot_of) & (col_of // 4 == slot_of - 48 * frag_of)).astype(F32)
    stacked = contract(pick, pot_all[...].reshape(192, 48), ((1,), (0,)))
    spread = (iota((48, N), 1) % 48 == iota((48, N), 0)).astype(F32)
    wide = contract(stacked, spread, ((1,), (0,)))
    rows, cols = iota((N, N), 0), iota((N, N), 1)
    wide = jnp.where(rows // 48 == cols // 48, wide, 0.0)
    wide = 0.5 * (wide + wide.T)
    place = (rows == imp_flat[...].reshape(1, N)).astype(F32)
    u_ref[...] = contract(contract(place, wide, ((1,), (0,))), place, ((1,), (1,)))

    for step in (1, 2, 3):
        remote(
            m_src.at[0], m_all.at[(orb + 4 - step) % 4], s_fock.at[step], r_fock.at[step], ka, orb
        ).wait_recv()
    m = m_all[...].reshape(N, N)
    mt = m.T
    scale = 1.0 / bound[0]
    eye = (rows == cols).astype(F32)
    x_out[:, :N] = (0.5 * (m + mt) + u_ref[...] - chem[0] * eye) * scale
    x_out[:, N:] = (0.5 * (m - mt)) * scale
    for step in (1, 2, 3):
        remote(pot, pot_all.at[0], s_pot.at[step], r_pot.at[step], ka, orb).wait_send()
        remote(m_src.at[0], m_all.at[0], s_fock.at[step], r_fock.at[step], ka, orb).wait_send()


def main_kernel(
    x_in, imp_hbm, t_hi, t_lo, landing, f_in,
    imp_flat,
    x_ref, w_hi, w_lo, d_tiles, k_buf, o_buf, d0_buf, full, f_out,
    s_imp, entered, s_k, r_k, s_o, r_o, s_d0, r_d0, s_f, r_f,
):
    ka = lax.axis_index("ka")
    orb = lax.axis_index("orb")
    z, x, yl = ka // 8, (ka // 2) % 4, ka % 2
    yh, core = orb // 2, orb % 2
    me = ka * 4 + orb
    barrier = pltpu.get_barrier_semaphore()

    def greet(d, carry):
        plane = (ka + d // 4) % 8
        pl.semaphore_signal(barrier, inc=1, device_id=(8 * z + plane, (orb + d) % 4), device_id_type=MESH)
        return carry

    fetch = pltpu.make_async_copy(imp_hbm, imp_flat, s_imp)
    fetch.start()
    lax.fori_loop(1, 32, greet, 0)
    for step in range(1, 8):
        pl.semaphore_signal(barrier, inc=1, device_id=((ka + 8 * step) % 64, orb), device_id_type=MESH)

    x_ref[...] = x_in[...]
    rows, cols = iota((N, N), 0), iota((N, N), 1)
    eye = (rows == cols).astype(F32)
    for step in range(ITERS):
        hi, lo = split2(x_ref[...])
        for part, w in ((hi, w_hi), (lo, w_lo)):
            w[:N, :N] = part[:, :N]
            w[:N, N:] = part[:, N:]
            w[N:, :N] = -part[:, N:]
            w[N:, N:] = part[:, :N]
        s = dot3(hi, lo, w_hi[...], w_lo[...])
        s_hi, s_lo = split2(s)
        c = dot3(s_hi, s_lo, w_hi[...], w_lo[...])
        x_ref[...] = 1.5 * x_ref[...] - 0.5 * c
        if step == 0:
            fetch.wait()
            pl.semaphore_wait(barrier, 38)
            for hop in range(1, 8):
                pl.semaphore_signal(entered, inc=1, device_id=((ka + 8 * hop) % 64, orb), device_id_type=MESH)
    slot_of_tile = slots()
    values = (0.5 * eye - 0.5 * x_ref[:, :N], -0.5 * x_ref[:, N:])
    for n, (o, p) in enumerate(PAIRS):
        re, im = (pack(v[96 * o : 96 * o + 96, 96 * p : 96 * p + 96]).reshape(9, 8, 128) for v in values)
        for half in range(2):
            rows_at = slice(4 * half, 4 * half + 4)
            quads = jnp.concatenate([re[:, rows_at], im[:, rows_at]], axis=1)
            for t in range(9):
                d_tiles[slot_of_tile[18 * n + 9 * half + t]] = quads[t]

    column = x * 4 + yh * 2 + yl
    turn = lax.rem(z + 16 - column, 8)
    first, first_slot, second, second_slot, has_second = own_tiles(turn, column)
    own_tile = jnp.where(core == 1, first, second)
    own_slot = jnp.where(core == 1, first_slot, second_slot)
    has_tile = (core == 1) | has_second
    pl.semaphore_wait(entered, 7)

    def send_k(slot, to_ka, to_orb):
        remote(d_tiles.at[slot], k_buf.at[me], s_k, r_k, to_ka, to_orb).start()

    def column_at(e):
        to_x = lax.rem(x + far_first(lax.rem(e, 4)), 4)
        to_y = lax.rem(2 * yh + yl + far_first(lax.div(e, 4)), 4)
        to_yh, to_yl = lax.div(to_y, 2), lax.rem(to_y, 2)
        return to_x * 4 + to_yh * 2 + to_yl, to_x * 2 + to_yl, to_yh * 2

    def spread_first(e, carry):
        to_column, to_line, to_orb = column_at(e)
        for step in STEPS:
            to_z = lax.rem(z + step, 8)
            slot = lax.rem(to_z + 16 - to_column, 8) * 16 + to_column
            if step:
                send_k(slot, to_z * 8 + to_line, to_orb + 1)
            else:

                @pl.when((e < 15) | (core == 0))
                def _(slot=slot, to_z=to_z):
                    send_k(slot, to_z * 8 + to_line, to_orb + 1)

        return carry

    lax.fori_loop(0, 16, spread_first, 0)

    def spread_second(e, carry):
        to_column, to_line, to_orb = column_at(e)
        for n, to_turn in enumerate((7, 1, 5)):
            to_z = lax.rem(to_turn + to_column, 8)

            @pl.when((e < 15) | (core == 1) | (to_z != z))
            def _(n=n, to_z=to_z):
                send_k(128 + 16 * n + to_column, to_z * 8 + to_line, to_orb)

        return carry

    def spread_late(e, carry):
        place = lax.rem(e + column, 4)
        to_column = 12 + place
        to_z = lax.rem(6 + to_column, 8)

        @pl.when((to_column != column) | (core == 1) | (to_z != z))
        def _():
            send_k(164 + to_column, to_z * 8 + 6 + lax.rem(place, 2), 2 * lax.div(place, 2))

        return carry

    lax.fori_loop(0, 4, spread_late, 0)
    lax.fori_loop(0, 16, spread_second, 0)
    t_o, t_p = blocks_of(own_tile // 18)
    t_m = own_tile % 18
    mirrored = t_o != t_p
    to_self = (t_o == orb) | (t_p == orb)

    @pl.when(has_tile)
    def _():
        k_buf[me] = d_tiles[own_slot]
        wait_bytes(k_buf.at[pl.ds(0, K - 1)], r_k)
        k_rows = k_buf.reshape(K * 8, 128)
        o_rows = o_buf.reshape(2 * K * 8, 128)
        for s in range(4):
            both = [k_rows[pl.ds(c * 4 + s, K, stride=8), :] for c in range(2)]
            v_hi, v_lo = split2(jnp.concatenate(both, axis=1))
            res = dot3(t_hi[...], t_lo[...], v_hi, v_lo)
            cos_re, cos_im = res[:K, :128], res[:K, 128:]
            sin_re, sin_im = res[K:, :128], res[K:, 128:]
            o_rows[pl.ds(s, K, stride=8), :] = cos_re - sin_im
            o_rows[pl.ds(4 + s, K, stride=8), :] = cos_im + sin_re
            o_rows[pl.ds(K * 8 + s, K, stride=8), :] = cos_re + sin_im
            o_rows[pl.ds(K * 8 + 4 + s, K, stride=8), :] = sin_re - cos_im

        def send_d0(g, carry):
            to_ka, to_orb = frag_device(g)
            remote(o_buf.at[0, 0], d0_buf.at[own_tile], s_d0, r_d0, to_ka, to_orb).start()
            return carry

        lax.fori_loop(0, 12, send_d0, 0)

        def send_o(e, carry):
            to_x = lax.rem(x + far_first(lax.rem(e, 4)), 4)
            to_yl = lax.rem(yl + 1 - lax.div(e, 4), 2)
            to_line = to_x * 2 + to_yl

            def send_side(side, place, to_orb):
                for step in STEPS:
                    to_ka = lax.rem(z + step, 8) * 8 + to_line

                    def send(to_ka=to_ka):
                        cells_at = o_buf.at[side, pl.ds(4 * to_ka, 4)]
                        remote(cells_at, landing.at[place], s_o, r_o, to_ka, to_orb).start()

                    if step:
                        send()
                    else:
                        pl.when((e < 7) | (to_orb != orb))(send)

            send_side(0, t_p * 18 + t_m, t_o)

            @pl.when(mirrored)
            def _():
                send_side(1, t_o * 18 + t_m, t_p)

            return carry

        lax.fori_loop(0, 8, send_o, 0)

        @pl.when(t_o == orb)
        def _():
            landing[t_p * 18 + t_m] = o_buf[0, pl.ds(4 * ka, 4)]

        @pl.when(mirrored & (t_p == orb))
        def _():
            landing[t_o * 18 + t_m] = o_buf[1, pl.ds(4 * ka, 4)]

    f_o, f_part = lax.rem(column + 1, 4), lax.div(column, 4)
    makes = (core == 0) & (turn == 3) & (column < 12)

    @pl.when(makes)
    def _():
        imp = imp_flat[...].reshape(1, N)
        slots = [imp[:, 96 * o : 96 * o + 96] for o in range(4)]
        own_slots = slots[0]
        for o in range(1, 4):
            own_slots = jnp.where(f_o == o, slots[o], own_slots)
        own_slots = jnp.concatenate([own_slots, jnp.full((1, 32), -1, jnp.int32)], axis=1)
        wait_bytes(d0_buf, r_d0)
        chosen = (iota((N, 128), 0) == own_slots).astype(F32)
        left = iota((48, 128), 1) < 48
        for part in range(2):
            for n, (o, p) in enumerate(PAIRS):
                halves = [d0_buf[18 * n + 9 * h : 18 * n + 9 * h + 9, 4 * part : 4 * part + 4] for h in range(2)]
                block = unpack(jnp.concatenate(halves, axis=1).reshape(72, 128))
                full[96 * o : 96 * o + 96, 96 * p : 96 * p + 96] = block
                if o != p:
                    full[96 * p : 96 * p + 96, 96 * o : 96 * o + 96] = block.T if part == 0 else -block.T
            picked = contract(contract(chosen, full[...], ((0,), (0,))), chosen, ((1,), (0,)))
            f_out[part] = jnp.where(left, picked[:48], picked[48:96])

        def send_f(d, carry):
            to_ka = lax.rem(z + lax.rem(d * 3 + 4, 8), 8) * 8 + lax.rem(ka + lax.div(d, 8), 8)
            rows_at = pl.ds(pl.multiple_of(16 * f_part, 8), 16)
            remote(f_out.at[:, rows_at], f_in.at[:, rows_at], s_f, r_f, to_ka, f_o).start()
            return carry

        lax.fori_loop(0, 64, send_f, 0)

    wait_bytes(f_in, r_f)
    keeps = has_tile & to_self

    @pl.when(keeps)
    def _():
        wait_bytes(landing.at[pl.ds(0, 71)], r_o)

    @pl.when(jnp.logical_not(keeps))
    def _():
        wait_bytes(landing, r_o)

    @pl.when(has_tile)
    def _():
        wait_bytes(d_tiles.at[pl.ds(0, TILES - 1)], s_k)
        wait_bytes(d_tiles.at[pl.ds(0, 12)], s_d0)

    @pl.when(jnp.logical_not(has_tile))
    def _():
        wait_bytes(d_tiles, s_k)

    for side, sent, fewer in (
        (mirrored, o_buf, o_buf.at[:, pl.ds(0, K - 2)]),
        (jnp.logical_not(mirrored), o_buf.at[0], o_buf.at[0, pl.ds(0, K - 4)]),
    ):

        @pl.when(has_tile & side & to_self)
        def _(fewer=fewer):
            wait_bytes(fewer, s_o)

        @pl.when(has_tile & side & jnp.logical_not(to_self))
        def _(sent=sent):
            wait_bytes(sent, s_o)

    @pl.when(makes)
    def _():
        wait_bytes(k_buf, s_f)


def store_kernel(landing, f_in, out, frag, buf, sem):
    own = lax.axis_index("orb")
    stores = [
        [pltpu.make_async_copy(buf.at[c, r], out.at[c, r], sem.at[c, r]) for r in range(4)] for c in range(2)
    ]
    for place in range(4):

        @pl.when(own == place)
        def _(place=place):
            for r in range(4):
                for c in range(2):
                    blocks = []
                    for q in range(4):
                        halves = [
                            landing[18 * q + 9 * h : 18 * q + 9 * h + 9, r, 4 * c : 4 * c + 4] for h in range(2)
                        ]
                        block = unpack(jnp.concatenate(halves, axis=1).reshape(72, 128))
                        blocks.append(block if place <= q else block.T)
                    buf[c, r] = jnp.concatenate(blocks, axis=1)
                    stores[c][r].start()

    for part in range(2):
        for f in range(2):
            frag[part, f] = f_in[part, :, 48 * f : 48 * f + 48]
    for store in stores[0] + stores[1]:
        store.wait()


def tables():
    grid = np.outer(np.arange(K), np.arange(K)) % K
    angle = grid * (2.0 * math.pi / K)
    c, s = np.cos(angle) / K, np.sin(angle) / K
    full = np.concatenate([c, s]).astype(np.float32)
    hi = full.astype(jnp.bfloat16)
    lo = (full - hi.astype(np.float32)).astype(jnp.bfloat16)
    return hi, lo


def per_device(fock, potential, chem_potential, spectral_bound, impurity_orbitals, potential_of):
    t_hi, t_lo = tables()
    vmem = pl.BlockSpec(memory_space=pltpu.VMEM)
    smem = pl.BlockSpec(memory_space=pltpu.SMEM)
    hbm = pl.BlockSpec(memory_space=pltpu.HBM)
    dma = pltpu.SemaphoreType.DMA
    pot = potential.transpose(1, 0, 2).reshape(48, 48)
    imp = pltpu.with_memory_space_constraint(impurity_orbitals, pltpu.HBM)
    start = pl.pallas_call(
        gather_kernel,
        name="gather",
        out_shape=jax.ShapeDtypeStruct((N, 2 * N), F32),
        in_specs=[hbm, hbm, smem, smem, hbm, hbm],
        out_specs=vmem,
        scratch_shapes=[
            pltpu.VMEM((2, 4, 96, N), F32),
            pltpu.VMEM((48, 48), F32),
            pltpu.VMEM((N,), jnp.int32),
            pltpu.SMEM((8,), jnp.int32),
            pltpu.VMEM((4, 96, N), F32),
            pltpu.VMEM((4, 96, N), F32),
            pltpu.VMEM((4, 48, 48), F32),
            pltpu.VMEM((N, N), F32),
            dma((7,)), dma((4,)), dma((4,)), dma((4,)), dma((4,)),
        ],
        compiler_params=pltpu.CompilerParams(
            has_side_effects=True, collective_id=0, vmem_limit_bytes=40 << 20
        ),
    )(
        pltpu.with_memory_space_constraint(fock, pltpu.HBM),
        pltpu.with_memory_space_constraint(pot, pltpu.HBM),
        chem_potential,
        spectral_bound,
        imp,
        pltpu.with_memory_space_constraint(potential_of, pltpu.HBM),
    )
    landing, f_in = pl.pallas_call(
        main_kernel,
        name="transform",
        out_shape=(
            jax.ShapeDtypeStruct((72, 4, 8, 128), F32),
            jax.ShapeDtypeStruct((2, 48, 128), F32),
        ),
        in_specs=[vmem, hbm, vmem, vmem],
        out_specs=(vmem, vmem),
        scratch_shapes=[
            pltpu.VMEM((N,), jnp.int32),
            pltpu.VMEM((N, 2 * N), F32),
            pltpu.VMEM((2 * N, 2 * N), BF16),
            pltpu.VMEM((2 * N, 2 * N), BF16),
            pltpu.VMEM((TILES, 8, 128), F32),
            pltpu.VMEM((K, 8, 128), F32),
            pltpu.VMEM((2, K, 8, 128), F32),
            pltpu.VMEM((TILES, 8, 128), F32),
            pltpu.VMEM((N, N), F32),
            pltpu.VMEM((2, 48, 128), F32),
            dma,
            pltpu.SemaphoreType.REGULAR,
            dma, dma, dma, dma, dma, dma, dma, dma,
        ],
        compiler_params=pltpu.CompilerParams(
            has_side_effects=True, collective_id=1, vmem_limit_bytes=48 << 20
        ),
    )(start, imp, jnp.asarray(t_hi), jnp.asarray(t_lo))
    return pl.pallas_call(
        store_kernel,
        name="store",
        out_shape=(
            jax.ShapeDtypeStruct((2, 4, 96, N), F32),
            jax.ShapeDtypeStruct((2, 2, 48, 48), F32),
        ),
        in_specs=[vmem, vmem],
        out_specs=(hbm, vmem),
        scratch_shapes=[pltpu.VMEM((2, 4, 96, N), F32), dma((2, 4))],
        compiler_params=pltpu.CompilerParams(vmem_limit_bytes=8 << 20),
    )(landing, f_in)


def solution(mesh):
    return jax.shard_map(
        per_device,
        mesh=mesh,
        in_specs=(P(None, "ka", "orb", None), P(None, "orb", None), P(), P(), P(), P()),
        out_specs=(P(None, "ka", "orb", None), P(None, "orb", None, None)),
        check_vma=False,
    )
```
